32 devices in a mesh: rep: 4 (over x, y), dp: 8 (over z, core).
Axes of the slice: x: 2, y: 2, z: 4, core: 2. Of those that a mesh axis runs over, the one named last changes fastest.
Arguments:
- x: bfloat16 [32, 2048, 512], P(('rep', 'dp')), parts along dimension 0
- dy: bfloat16 [32, 2048, 512], P(('rep', 'dp')), parts along dimension 0
- wq: bfloat16 [2, 512, 512], replicated
- wk: bfloat16 [2, 512, 512], replicated
- wv: bfloat16 [2, 512, 512], replicated
- wo: bfloat16 [2, 512, 512], replicated
- w_gate: bfloat16 [2, 512, 2048], replicated
- w_up: bfloat16 [2, 512, 2048], replicated
- w_down: bfloat16 [2, 2048, 512], replicated
- m_wq: float32 [2, 512, 512], replicated
- m_wk: float32 [2, 512, 512], replicated
- m_wv: float32 [2, 512, 512], replicated
- m_wo: float32 [2, 512, 512], replicated
- m_w_gate: float32 [2, 512, 2048], replicated
- m_w_up: float32 [2, 512, 2048], replicated
- m_w_down: float32 [2, 2048, 512], replicated
- v_wq: float32 [2, 512, 512], replicated
- v_wk: float32 [2, 512, 512], replicated
- v_wv: float32 [2, 512, 512], replicated
- v_wo: float32 [2, 512, 512], replicated
- v_w_gate: float32 [2, 512, 2048], replicated
- v_w_up: float32 [2, 512, 2048], replicated
- v_w_down: float32 [2, 2048, 512], replicated
Outputs:
- output 1: bfloat16 [8, 512, 512], P('rep'), parts along dimension 0
- output 2: bfloat16 [8, 512, 512], P('rep'), parts along dimension 0
- output 3: bfloat16 [8, 512, 512], P('rep'), parts along dimension 0
- output 4: bfloat16 [8, 512, 512], P('rep'), parts along dimension 0
- output 5: bfloat16 [8, 512, 2048], P('rep'), parts along dimension 0
- output 6: bfloat16 [8, 512, 2048], P('rep'), parts along dimension 0
- output 7: bfloat16 [8, 2048, 512], P('rep'), parts along dimension 0
- output 8: float32 [8, 512, 512], P('rep'), parts along dimension 0
- output 9: float32 [8, 512, 512], P('rep'), parts along dimension 0
- output 10: float32 [8, 512, 512], P('rep'), parts along dimension 0
- output 11: float32 [8, 512, 512], P('rep'), parts along dimension 0
- output 12: float32 [8, 512, 2048], P('rep'), parts along dimension 0
- output 13: float32 [8, 512, 2048], P('rep'), parts along dimension 0
- output 14: float32 [8, 2048, 512], P('rep'), parts along dimension 0
- output 15: float32 [8, 512, 512], P('rep'), parts along dimension 0
- output 16: float32 [8, 512, 512], P('rep'), parts along dimension 0
- output 17: float32 [8, 512, 512], P('rep'), parts along dimension 0
- output 18: float32 [8, 512, 512], P('rep'), parts along dimension 0
- output 19: float32 [8, 512, 2048], P('rep'), parts along dimension 0
- output 20: float32 [8, 512, 2048], P('rep'), parts along dimension 0
- output 21: float32 [8, 2048, 512], P('rep'), parts along dimension 0
There are 4 independent parts. The reference program is written for one: setup_inputs(seed, part) draws one part's arguments, and reference() takes and returns one part's arrays. A program takes and returns all parts, laid end to end along the dimension named above; an argument that names none is the same for every part.
All inputs are finite; a program needn't handle non-finite values.
Results may differ from the reference program's by a relative error of at most 0.024.
Values are sent between devices in bfloat16 or wider.
A program may use at most 2.25 GiB of HBM per device.

```python
import jax
import jax.numpy as jnp
from jax import lax

SEQUENCES = 8
TOKENS = 2048
D = 512
HEADS = 2
KV_HEADS = 2
HEAD = 256
FF = 2048
LAYERS = 2
THETA = 10000
NAMES = ("wq", "wk", "wv", "wo", "w_gate", "w_up", "w_down")
SHAPES = {
    "wq": (LAYERS, D, HEADS * HEAD),
    "wk": (LAYERS, D, KV_HEADS * HEAD),
    "wv": (LAYERS, D, KV_HEADS * HEAD),
    "wo": (LAYERS, HEADS * HEAD, D),
    "w_gate": (LAYERS, D, FF),
    "w_up": (LAYERS, D, FF),
    "w_down": (LAYERS, FF, D),
}


def bump(key, n, height):
    away = (jnp.arange(n, dtype=jnp.int32) - jax.random.randint(key, (), 0, n, jnp.int32)) % n
    return jnp.where(away < n // 8, height, 1.0)


def together(key, own, strength):
    shared = jax.random.normal(key, own.shape[1:], jnp.float32)
    return (own + strength * shared) * lax.rsqrt(1 + strength * strength)


def setup_inputs(seed: int = 0, part: int = 0) -> dict:
    kx, kdy, ka, kb, kz, kf, kh, kl, *keys = jax.random.split(jax.random.key(seed), 8 + 3 * len(NAMES))
    kx, kdy, ka, kb = (jax.random.fold_in(k, part) for k in (kx, kdy, ka, kb))
    kw, km, kv = (keys[i::3] for i in range(3))
    shape = (SEQUENCES, TOKENS, D)
    much_x, much_dy = jax.random.uniform(kz, (2,), jnp.float32, 0.0, 1.0)
    loud = 2.0 ** jax.random.uniform(jax.random.fold_in(kz, 1), (), jnp.float32, -1.0, 2.0)
    layers = 2.0 ** jax.random.uniform(kl, (LAYERS, 1, 1), jnp.float32, -1.0, 1.0)
    times = {"wq": 1.0, "wk": 1.0, "wv": 2.0, "wo": layers, "w_gate": 1.0, "w_up": bump(kh, FF, 4.0), "w_down": layers}
    x = together(ka, jax.random.normal(kx, shape, jnp.float32), much_x) * bump(kf, D, 4.0)
    dy = together(kb, jax.random.normal(kdy, shape, jnp.float32), much_dy)
    drawn = {"x": x.astype(jnp.bfloat16), "dy": (loud * dy * (SEQUENCES * TOKENS) ** -0.5).astype(jnp.bfloat16)}
    for key, name in zip(kw, NAMES, strict=True):
        drawn[name] = (jax.random.normal(key, SHAPES[name], jnp.float32) * SHAPES[name][1] ** -0.5 * times[name]).astype(jnp.bfloat16)
    for key, name in zip(km, NAMES, strict=True):
        drawn[f"m_{name}"] = 0.1 * jax.random.normal(key, SHAPES[name], jnp.float32)
    for key, name in zip(kv, NAMES, strict=True):
        drawn[f"v_{name}"] = jax.random.uniform(key, SHAPES[name], jnp.float32, 0.02, 0.06)
    return drawn


def matmul(a, w):
    return jnp.dot(a, w, preferred_element_type=jnp.float32).astype(jnp.bfloat16)


def normed(h):
    wide = h.astype(jnp.float32)
    scale = lax.rsqrt(jnp.mean(wide**2, -1, keepdims=True) + 1e-6)
    return (wide * scale).astype(jnp.bfloat16)


def turned(t, theta):
    half = t.shape[-1] // 2
    angle = jnp.arange(t.shape[0], dtype=jnp.float32)[:, None] * theta ** (-jnp.arange(half, dtype=jnp.float32) / half)
    cos, sin = jnp.cos(angle)[:, None], jnp.sin(angle)[:, None]
    a, b = t[..., :half].astype(jnp.float32), t[..., half:].astype(jnp.float32)
    return jnp.concatenate([a * cos - b * sin, b * cos + a * sin], -1).astype(jnp.bfloat16)


def seen_by(q, k, v):
    tokens, kv = q.shape[0], k.shape[1]
    q = q.reshape(tokens, kv, -1, q.shape[-1])
    scores = jnp.einsum("tgsd,ugd->gstu", q.astype(jnp.float32), k.astype(jnp.float32)) * q.shape[-1] ** -0.5
    place = jnp.arange(tokens)
    weights = jax.nn.softmax(jnp.where(place[:, None] >= place, scores, -jnp.inf), -1).astype(jnp.bfloat16)
    return jnp.einsum("gstu,ugd->tgsd", weights.astype(jnp.float32), v.astype(jnp.float32)).astype(jnp.bfloat16).reshape(tokens, -1)


def layer(h, w):
    a = normed(h)
    q, k = (turned(matmul(a, w[name]).reshape(h.shape[0], -1, HEAD), THETA) for name in ("wq", "wk"))
    h = h + matmul(seen_by(q, k, matmul(a, w["wv"]).reshape(h.shape[0], -1, HEAD)), w["wo"])
    b = normed(h)
    gate = jnp.dot(b, w["w_gate"], preferred_element_type=jnp.float32)
    up = jnp.dot(b, w["w_up"], preferred_element_type=jnp.float32)
    return h + matmul((jax.nn.silu(gate) * up).astype(jnp.bfloat16), w["w_down"])


def adamw(w, m, v, g):
    m = 0.9 * m + 0.1 * g
    v = 0.95 * v + 0.05 * g * g
    step = m * lax.rsqrt(v + 1e-8) + 0.1 * w
    return (w - 0.02 * step).astype(jnp.bfloat16), m, v


def clipped(gradients, sum_of_squares, count):
    factor = jnp.minimum(1.0, 0.5 * lax.rsqrt(sum_of_squares / count + 1e-30))
    return [g * factor for g in gradients]


def stack(weights, h):
    return lax.scan(lambda h, w: (layer(h, w), None), h, weights)[0]


def reference(x, dy, wq, wk, wv, wo, w_gate, w_up, w_down, m_wq, m_wk, m_wv, m_wo, m_w_gate, m_w_up, m_w_down, v_wq, v_wk, v_wv, v_wo, v_w_gate, v_w_up, v_w_down):
    weights = dict(zip(NAMES, (wq, wk, wv, wo, w_gate, w_up, w_down), strict=True))

    def take(so_far, sequence):
        h, by_y = sequence
        _, back = jax.vjp(stack, weights, h)
        by_weights, by_h = back(by_y)
        return jax.tree.map(lambda total, term: total + term.astype(jnp.float32), so_far, by_weights), by_h

    none_yet = {name: jnp.zeros(w.shape, jnp.float32) for name, w in weights.items()}
    by_weights, by_x = lax.scan(take, none_yet, (x, dy))
    gradients = [by_weights[name].astype(jnp.bfloat16).astype(jnp.float32) for name in NAMES]
    gradients = clipped(gradients, sum(jnp.sum(g * g) for g in gradients), sum(g.size for g in gradients))
    first = (m_wq, m_wk, m_wv, m_wo, m_w_gate, m_w_up, m_w_down)
    second = (v_wq, v_wk, v_wv, v_wo, v_w_gate, v_w_up, v_w_down)
    new = [adamw(weights[name].astype(jnp.float32), m, v, g) for name, m, v, g in zip(NAMES, first, second, gradients, strict=True)]
    return tuple(one[which] for which in range(3) for one in new)
```

```python
import functools

import jax
import jax.numpy as jnp
from jax import lax
from jax.experimental import pallas as pl
from jax.experimental.pallas import tpu as pltpu
from jax.sharding import PartitionSpec as P

BF, F32 = jnp.bfloat16, jnp.float32
LOG2E = 1.4426950408889634
HEAD = 256
THETA = 10000
HALF = HEAD // 2
TILE = 512
FB = 512
VMEM = 60 * 2**20


def _dot(a, b, ca=1, cb=0):
    return lax.dot_general(a, b, (((ca,), (cb,)), ((), ())), preferred_element_type=F32)


def _norm(h):
    wide = h.astype(F32)
    scale = lax.rsqrt(jnp.mean(wide * wide, -1, keepdims=True) + 1e-6)
    return (wide * scale).astype(BF), wide, scale


def _norm_back(by_out, wide, scale):
    by_scale = jnp.sum(by_out * wide, -1, keepdims=True)
    return by_out * scale - wide * (by_scale * scale * scale * scale * (1.0 / wide.shape[-1]))


def _turn(t, cos, sin, back=False):
    a, b = t[:, :HALF].astype(F32), t[:, HALF:].astype(F32)
    if back:
        return jnp.concatenate([a * cos + b * sin, b * cos - a * sin], -1).astype(BF)
    return jnp.concatenate([a * cos - b * sin, b * cos + a * sin], -1).astype(BF)


def _params(semantics, **more):
    return pltpu.CompilerParams(dimension_semantics=semantics, vmem_limit_bytes=VMEM, **more)


def _cost(flops, bytes_, exps=0):
    return pl.CostEstimate(flops=int(flops), bytes_accessed=int(bytes_), transcendentals=int(exps))


def _qkv_kernel(h_ref, wq_ref, wk_ref, wv_ref, cos_ref, sin_ref, q_ref, k_ref, v_ref):
    a, _, _ = _norm(h_ref[...])
    cos, sin = cos_ref[...], sin_ref[...]
    for w_ref, out in ((wq_ref, q_ref), (wk_ref, k_ref)):
        t = _dot(a, w_ref[0]).astype(BF)
        for at in range(0, t.shape[1], HEAD):
            out[:, at : at + HEAD] = _turn(t[:, at : at + HEAD], cos, sin)
    v_ref[...] = _dot(a, wv_ref[0]).astype(BF)


def _qkv(h, wq, wk, wv, cos, sin, layer):
    t, d = h.shape
    rows = pl.BlockSpec((TILE, d), lambda i: (i, 0))
    whole = pl.BlockSpec((1, d, d), lambda i: (layer, 0, 0))
    table = pl.BlockSpec((TILE, HALF), lambda i: (i, 0))
    return pl.pallas_call(
        _qkv_kernel,
        grid=(t // TILE,),
        in_specs=[rows, whole, whole, whole, table, table],
        out_specs=[rows] * 3,
        out_shape=[jax.ShapeDtypeStruct((t, d), BF)] * 3,
        compiler_params=_params(("arbitrary",)),
        cost_estimate=_cost(6 * t * d * d, 8 * t * d + 6 * d * d),
        name="qkv",
    )(h, wq, wk, wv, cos, sin)


def _attend_kernel(q_ref, k_ref, v_ref, o_ref, lse_ref, vt_s, p_s):
    t = q_ref.shape[0]
    e = HEAD**-0.5 * LOG2E
    vt_s[...] = v_ref[...].T
    hide = lax.broadcasted_iota(jnp.int32, (TILE, TILE), 0) > lax.broadcasted_iota(jnp.int32, (TILE, TILE), 1)
    for at in range(0, t, TILE):
        q = q_ref[at : at + TILE, :]
        scores = [_dot(k_ref[j : j + TILE, :], q, 1, 1) for j in range(0, at + TILE, TILE)]
        scores[-1] = jnp.where(hide, -jnp.inf, scores[-1])
        top = functools.reduce(jnp.maximum, [s.max(axis=0, keepdims=True) for s in scores])
        total = 0.0
        for n, s in enumerate(scores):
            p = jnp.exp2((s - top) * e)
            total = total + p.sum(axis=0, keepdims=True)
            p_s[n * TILE : (n + 1) * TILE, :] = p.astype(BF)
        mix = _dot(vt_s[:, : at + TILE], p_s[: at + TILE, :])
        o_ref[at : at + TILE, :] = (mix * (1.0 / total)).T.astype(BF)
        lse_ref[0, :, at : at + TILE] = top * e + jnp.log2(total)


def _attend(q, k, v):
    t, d = q.shape
    head = pl.BlockSpec((t, HEAD), lambda h: (0, h))
    return pl.pallas_call(
        _attend_kernel,
        grid=(d // HEAD,),
        in_specs=[head] * 3,
        out_specs=[head, pl.BlockSpec((1, 1, t), lambda h: (h, 0, 0))],
        out_shape=[jax.ShapeDtypeStruct((t, d), BF), jax.ShapeDtypeStruct((d // HEAD, 1, t), F32)],
        scratch_shapes=[pltpu.VMEM((HEAD, t), BF), pltpu.VMEM((t, TILE), BF)],
        compiler_params=_params(("arbitrary",)),
        cost_estimate=_cost(2.5 * t * t * d, 8 * t * d, t * t),
        name="attend",
    )(q, k, v)


def _mix_kernel(h_ref, o_ref, wo_ref, h2_ref):
    h2_ref[...] = h_ref[...] + _dot(o_ref[...], wo_ref[0]).astype(BF)


def _mix(h, o, wo, layer):
    t, d = h.shape
    rows = pl.BlockSpec((TILE, d), lambda i: (i, 0))
    return pl.pallas_call(
        _mix_kernel,
        grid=(t // TILE,),
        in_specs=[rows, rows, pl.BlockSpec((1, d, d), lambda i: (layer, 0, 0))],
        out_specs=rows,
        out_shape=jax.ShapeDtypeStruct((t, d), BF),
        compiler_params=_params(("arbitrary",)),
        cost_estimate=_cost(2 * t * d * d, 6 * t * d),
        name="mix",
    )(h, o, wo)


def _feed_kernel(h_ref, o_ref, wo_ref, wg_ref, wu_ref, wd_ref, h2_ref, h3_ref):
    h2 = h_ref[...] + _dot(o_ref[...], wo_ref[0]).astype(BF)
    h2_ref[...] = h2
    b, _, _ = _norm(h2)
    out = 0.0
    for at in range(0, wg_ref.shape[2], FB):
        gate, up = _dot(b, wg_ref[0, :, at : at + FB]), _dot(b, wu_ref[0, :, at : at + FB])
        act = (gate * jax.nn.sigmoid(gate) * up).astype(BF)
        out = out + _dot(act, wd_ref[0, at : at + FB, :])
    h3_ref[...] = h2 + out.astype(BF)


def _feed(h, o, wo, wg, wu, wd, layer):
    t, d = h.shape
    f = wg.shape[2]
    rows = pl.BlockSpec((TILE, d), lambda i: (i, 0))
    whole = lambda *shape: pl.BlockSpec((1, *shape), lambda i: (layer, 0, 0))
    return pl.pallas_call(
        _feed_kernel,
        grid=(t // TILE,),
        in_specs=[rows, rows, whole(d, d), whole(d, f), whole(d, f), whole(f, d)],
        out_specs=[rows, rows],
        out_shape=[jax.ShapeDtypeStruct((t, d), BF)] * 2,
        compiler_params=_params(("arbitrary",)),
        cost_estimate=_cost(2 * t * d * d + 6 * t * d * f, 8 * t * d + 6 * d * f, t * f),
        name="feed",
    )(h, o, wo, wg, wu, wd)


def _feed_back_kernel(first, last, *refs):
    h2_ref, dh_ref, wg_ref, wu_ref, wd_ref = refs[:5]
    sum_in = None if first else refs[5]
    g_ref, out_ref, b_s, bt_s, dht_s, db_s, dgate_s, dup_s, act_s = refs[5 if first else 6 :]
    n = pl.program_id(0)
    t = h2_ref.shape[0]

    @pl.when(n == 0)
    def _():
        for at in range(0, t, TILE):
            b, _, _ = _norm(h2_ref[at : at + TILE, :])
            b_s[at : at + TILE, :] = b
            bt_s[:, at : at + TILE] = b.T
            dht_s[:, at : at + TILE] = dh_ref[at : at + TILE, :].T
            db_s[at : at + TILE, :] = jnp.zeros_like(db_s[at : at + TILE, :]) if first else sum_in[at : at + TILE, :]

    wg, wu, wd = wg_ref[0], wu_ref[0], wd_ref[0]
    for at in range(0, t, TILE):
        b = b_s[at : at + TILE, :]
        gate, up = _dot(b, wg), _dot(b, wu)
        dact = _dot(dh_ref[at : at + TILE, :], wd, 1, 1).astype(BF).astype(F32)
        sig = jax.nn.sigmoid(gate)
        silu = gate * sig
        act_s[at : at + TILE, :] = (silu * up).astype(BF)
        dup = (dact * silu).astype(BF)
        dgate = (dact * up * (sig + silu * (1.0 - sig))).astype(BF)
        dup_s[at : at + TILE, :] = dup
        dgate_s[at : at + TILE, :] = dgate
        db_s[at : at + TILE, :] += _dot(dgate, wg, 1, 1) + _dot(dup, wu, 1, 1)
    g_ref[0, 0] = _dot(bt_s[...], dgate_s[...]).astype(BF)
    g_ref[0, 1] = _dot(bt_s[...], dup_s[...]).astype(BF)
    g_ref[0, 2] = _dot(dht_s[...], act_s[...]).T.astype(BF)

    @pl.when(n == pl.num_programs(0) - 1)
    def _():
        for at in range(0, t, TILE):
            here = slice(at, at + TILE)
            if last:
                _, wide, scale = _norm(h2_ref[here, :])
                out_ref[here, :] = dh_ref[here, :] + _norm_back(db_s[here, :], wide, scale).astype(BF)
            else:
                out_ref[here, :] = db_s[here, :]


def _feed_back(h2, dh, wg, wu, wd, layer, start, count, so_far, last):
    t, d = h2.shape
    first = so_far is None
    whole = pl.BlockSpec((t, d), lambda n: (0, 0))
    columns = pl.BlockSpec((1, d, FB), lambda n: (layer, 0, start + n))
    in_specs = [whole, whole, columns, columns, pl.BlockSpec((1, FB, d), lambda n: (layer, start + n, 0))]
    given = [h2, dh, wg, wu, wd]
    if not first:
        in_specs, given = [*in_specs, whole], [*given, so_far]
    return pl.pallas_call(
        functools.partial(_feed_back_kernel, first, last),
        grid=(count,),
        in_specs=in_specs,
        out_specs=[pl.BlockSpec((1, 3, d, FB), lambda n: (n, 0, 0, 0)), whole],
        out_shape=[jax.ShapeDtypeStruct((count, 3, d, FB), BF), jax.ShapeDtypeStruct((t, d), BF if last else F32)],
        scratch_shapes=[pltpu.VMEM((t, d), BF), pltpu.VMEM((d, t), BF), pltpu.VMEM((d, t), BF), pltpu.VMEM((t, d), F32),
                        pltpu.VMEM((t, FB), BF), pltpu.VMEM((t, FB), BF), pltpu.VMEM((t, FB), BF)],
        compiler_params=_params(("arbitrary",)),
        cost_estimate=_cost(count * 16 * t * d * FB, 14 * t * d + count * 12 * d * FB, count * t * FB),
        name="feed_back",
    )(*given)


def _attend_back_kernel(with_dh, *refs):
    q_ref, k_ref, v_ref, o_ref, lse_ref, dh_ref, h_ref, wo_ref, wq_ref, wk_ref, wv_ref, cos_ref, sin_ref, g_ref = refs[:14]
    out_ref = refs[14] if with_dh else None
    do_s, at_s, dqt_s, da_s = refs[15 if with_dh else 14 :]
    n = pl.program_id(0)
    t = q_ref.shape[0]
    scale = HEAD**-0.5
    e = scale * LOG2E

    @pl.when(n == 0)
    def _():
        for at in range(0, t, TILE):
            at_s[:, at : at + TILE] = _norm(h_ref[at : at + TILE, :])[0].T

    deltas = []
    for at in range(0, t, TILE):
        here = slice(at, at + TILE)
        do = _dot(dh_ref[here, :], wo_ref[0], 1, 1).astype(BF)
        do_s[here, :] = do
        both = do.astype(F32) * o_ref[here, :].astype(F32)
        deltas.append((both[:, :HALF] + both[:, HALF:]).T.sum(axis=0, keepdims=True))
    delta = jnp.concatenate(deltas, axis=1)
    dwo = _dot(o_ref[...].T, dh_ref[...]).astype(BF)
    g_ref[0, 3, 0] = dwo[:, :HEAD]
    g_ref[0, 3, 1] = dwo[:, HEAD:]

    hide = lax.broadcasted_iota(jnp.int32, (TILE, TILE), 0) > lax.broadcasted_iota(jnp.int32, (TILE, TILE), 1)
    dks, dvs = [], []
    for at in range(0, t, TILE):
        k, v = k_ref[at : at + TILE, :], v_ref[at : at + TILE, :]
        kt = k.T
        ps, dss = [], []
        for i in range(at, t, TILE):
            here = slice(i, i + TILE)
            p = jnp.exp2(_dot(k, q_ref[here, :], 1, 1) * e - lse_ref[0, :, here])
            if i == at:
                p = jnp.where(hide, 0.0, p)
            ds = (p * (_dot(v, do_s[here, :], 1, 1) - delta[:, here])).astype(BF)
            ps.append(p.astype(BF))
            dss.append(ds)
        p, ds = jnp.concatenate(ps, axis=1), jnp.concatenate(dss, axis=1)
        dvs.append(_dot(p, do_s[at:, :]).astype(BF))
        dks.append((_dot(ds, q_ref[at:, :]) * scale).astype(BF))
        dq = _dot(kt, ds)
        dqt_s[:, at:] = dq if at == 0 else dqt_s[:, at:] + dq

    for m, w_ref in enumerate((wq_ref, wk_ref, wv_ref)):
        parts = []
        for j, at in enumerate(range(0, t, TILE)):
            here = slice(at, at + TILE)
            if m == 0:
                part = (dqt_s[:, here] * scale).T.astype(BF)
            else:
                part = (dks, dvs)[m - 1][j]
            if m < 2:
                part = _turn(part, cos_ref[here, :], sin_ref[here, :], True)
            parts.append(part)
            if with_dh:
                da = _dot(part, w_ref[0], 1, 1)
                if m == 0:
                    da_s[here, :] = jnp.where(n == 0, da, da_s[here, :] + da)
                else:
                    da_s[here, :] += da
        dw = _dot(at_s[...], jnp.concatenate(parts, axis=0)).astype(BF)
        g_ref[0, m, 0] = dw[:HEAD, :]
        g_ref[0, m, 1] = dw[HEAD:, :]

    if with_dh:
        @pl.when(n == pl.num_programs(0) - 1)
        def _():
            for at in range(0, t, TILE):
                here = slice(at, at + TILE)
                _, wide, s = _norm(h_ref[here, :])
                out_ref[here, :] = dh_ref[here, :] + _norm_back(da_s[here, :], wide, s).astype(BF)


def _attend_back(q, k, v, o, lse, dh, h, wo, wq, wk, wv, cos, sin, layer, with_dh):
    t, d = h.shape
    heads = d // HEAD
    head = pl.BlockSpec((t, HEAD), lambda n: (0, n))
    whole = pl.BlockSpec((t, d), lambda n: (0, 0))
    table = pl.BlockSpec((t, HALF), lambda n: (0, 0))
    columns = pl.BlockSpec((1, d, HEAD), lambda n: (layer, 0, n))
    out_specs = [pl.BlockSpec((1, 4, 2, HEAD, HEAD), lambda n: (n, 0, 0, 0, 0))]
    out_shape = [jax.ShapeDtypeStruct((heads, 4, 2, HEAD, HEAD), BF)]
    if with_dh:
        out_specs, out_shape = [*out_specs, whole], [*out_shape, jax.ShapeDtypeStruct((t, d), BF)]
    return pl.pallas_call(
        functools.partial(_attend_back_kernel, with_dh),
        grid=(heads,),
        in_specs=[head, head, head, head, pl.BlockSpec((1, 1, t), lambda n: (n, 0, 0)), whole, whole,
                  pl.BlockSpec((1, HEAD, d), lambda n: (layer, n, 0)), columns, columns, columns, table, table],
        out_specs=out_specs,
        out_shape=out_shape,
        scratch_shapes=[pltpu.VMEM((t, HEAD), BF), pltpu.VMEM((d, t), BF), pltpu.VMEM((HEAD, t), F32), pltpu.VMEM((t, d), F32)],
        compiler_params=_params(("arbitrary",)),
        cost_estimate=_cost(6.25 * t * t * d + (16 if with_dh else 10) * t * d * d, 16 * t * d, t * t),
        name="attend_back",
    )(q, k, v, o, lse, dh, h, wo, wq, wk, wv, cos, sin)


def _pairs(links, cores):
    return [(a * cores + c, b * cores + c) for a, b in links for c in range(cores)]


class _Sum:
    STAGES = 5

    def __init__(self, term):
        self.term, self.stage, self.sent = term, 0, None

    def start(self):
        me = lax.axis_index("dp")
        core, chip = me % 2, me // 2
        swap = [(i, i ^ 1) for i in range(8)]
        if self.stage == 0:
            self.mine = lax.dynamic_index_in_dim(self.term, core, 0, False)
            return lax.dynamic_index_in_dim(self.term, 1 - core, 0, False), swap
        if self.stage == 1:
            self.both = self.mine.astype(F32) + self.got.astype(F32)
            return self.both.astype(BF), _pairs([(0, 1), (3, 2)], 2)
        if self.stage == 2:
            self.side = (self.both + self.got.astype(F32)).astype(BF)
            return self.side, _pairs([(1, 2), (2, 1)], 2)
        if self.stage == 3:
            self.total = (self.side.astype(F32) + self.got.astype(F32)).astype(BF)
            return self.total, _pairs([(1, 0), (2, 3)], 2)
        self.mine = jnp.where((chip == 1) | (chip == 2), self.total, self.got)
        return self.mine, swap

    def finish(self, got):
        self.got, self.stage = got, self.stage + 1

    def result(self):
        core = lax.axis_index("dp") % 2
        return jnp.where(core == 0, jnp.stack([self.mine, self.got]), jnp.stack([self.got, self.mine]))


def _slot(sums, run, *given):
    live = [s for s in sums if s.stage < s.STAGES]
    sends = [s.start() for s in live]
    if sends:
        parts, given = lax.optimization_barrier(([x for x, _ in sends], given))
        sends = [(x, pairs) for x, (_, pairs) in zip(parts, sends)]
    got = [lax.ppermute(x, "dp", pairs) for x, pairs in sends]
    out = run(*given)
    if sends:
        got, out = lax.optimization_barrier((got, out))
    for s, g in zip(live, got):
        s.finish(g)
    return out


def _adamw_kernel(factor_ref, *refs):
    ins, outs = refs[:27], refs[27:]
    w_refs, m_refs, v_refs, gf, ga = ins[:7], ins[7:14], ins[14:21], ins[21:25], ins[25:27]
    factor = factor_ref[0]
    layer, f = pl.program_id(0), pl.program_id(1)
    part = layer * 2 + f // 2

    def one(i, g):
        m = 0.9 * m_refs[i][0] + 0.1 * g
        v = 0.95 * v_refs[i][0] + 0.05 * g * g
        w = w_refs[i][0].astype(F32)
        outs[i][0] = (w - 0.02 * (m * lax.rsqrt(v + 1e-8) + 0.1 * w)).astype(BF)
        outs[7 + i][0] = m
        outs[14 + i][0] = v

    for i in range(4):
        g = jnp.where(layer == 0, ga[0][0, i, 0], ga[1][0, i, 0]).astype(F32)
        one(i, g * factor)
    for i in range(3):
        g = jnp.where(part < 2, jnp.where(part == 0, gf[0][0, i], gf[1][0, i]), jnp.where(part == 2, gf[2][0, i], gf[3][0, i])).astype(F32)
        one(4 + i, g * factor)


def _adamw(factor, weights, m, v, feeds, attends):
    layers, d = weights[0].shape[:2]
    f = weights[4].shape[2]
    steps = f // FB
    rows, thin = FB // 2, HEAD // 2
    by_rows = pl.BlockSpec((1, thin, HEAD), lambda l, f, r, _: (l, (f % 2) * 2 + r, f // 2))
    by_columns = pl.BlockSpec((1, thin, HEAD), lambda l, f, r, _: (l, (f // 2) * 2 + r, f % 2))
    wide = pl.BlockSpec((1, rows, FB), lambda l, f, r, _: (l, r, f))
    down = pl.BlockSpec((1, rows, FB), lambda l, f, r, _: (l, 2 * f + r, 0))
    like = [by_rows, by_rows, by_rows, by_columns, wide, wide, down]

    def feed_spec(part):
        def index(l, f, r, _):
            at = l * steps + f - part * 2
            ok = (at >= 0) & (at < 2)
            return jnp.where(ok, at, jnp.where(at < 0, 0, 1)), 0, jnp.where(ok, r, jnp.where(at < 0, 0, 1)), 0

        return pl.BlockSpec((1, 3, rows, FB), index)

    def attend_spec(layer):
        def index(l, f, r, _):
            before, after = l < layer, l > layer
            pick = lambda x, top: jnp.where(before, 0, jnp.where(after, top, x))
            return pick(f // 2, 1), 0, pick(f % 2, 1), pick(r, 1), 0

        return pl.BlockSpec((1, 4, 1, thin, HEAD), index)

    outs = pl.pallas_call(
        _adamw_kernel,
        grid_spec=pltpu.PrefetchScalarGridSpec(
            num_scalar_prefetch=1,
            grid=(layers, steps, 2),
            in_specs=like * 3 + [feed_spec(i) for i in range(2 * layers)] + [attend_spec(i) for i in range(layers)],
            out_specs=like * 3,
        ),
        out_shape=[jax.ShapeDtypeStruct(w.shape, BF) for w in weights] + [jax.ShapeDtypeStruct(w.shape, F32) for w in weights] * 2,
        compiler_params=_params(("arbitrary",) * 3),
        cost_estimate=_cost(20 * layers * 8 * d * d, 22 * layers * (4 * d * d + 3 * d * f)),
        name="adamw",
    )(factor, *weights, *m, *v, *feeds, *attends)
    return tuple(outs)


def solution(mesh):
    def step(x, dy, *arrays):
        weights, m, v = (arrays[i : i + 7] for i in (0, 7, 14))
        wq, wk, wv, wo, wg, wu, wd = weights
        layers = wq.shape[0]
        h, t = x[0], x.shape[1]
        angle = jnp.arange(t, dtype=F32)[:, None] * THETA ** (-jnp.arange(HALF, dtype=F32) / HALF)
        cos, sin = jnp.cos(angle), jnp.sin(angle)
        kept = []
        for n in range(layers):
            q, k, val = _qkv(h, wq, wk, wv, cos, sin, n)
            o, lse = _attend(q, k, val)
            if n < layers - 1:
                h2, h3 = _feed(h, o, wo, wg, wu, wd, n)
            else:
                h2, h3 = _mix(h, o, wo, n), None
            kept.append((h, q, k, val, o, lse, h2))
            h = h3
        by_h = dy[0]
        feeds, attends = [None] * (2 * layers), [None] * layers
        sums = []
        for n in reversed(range(layers)):
            h, q, k, val, o, lse, h2 = kept[n]
            g, part = _slot(sums, lambda h2, by_h: _feed_back(h2, by_h, wg, wu, wd, n, 0, 2, None, False), h2, by_h)
            feeds[2 * n] = _Sum(g)
            sums.append(feeds[2 * n])
            g, by_h2 = _slot(sums, lambda h2, by_h, part: _feed_back(h2, by_h, wg, wu, wd, n, 2, 2, part, True), h2, by_h, part)
            feeds[2 * n + 1] = _Sum(g)
            sums.append(feeds[2 * n + 1])
            got = _slot(sums, lambda q, by_h2: _attend_back(q, k, val, o, lse, by_h2, h, wo, wq, wk, wv, cos, sin, n, n > 0), q, by_h2)
            attends[n] = _Sum(got[0])
            sums.append(attends[n])
            by_h = got[1] if n > 0 else None
        while any(s.stage < s.STAGES for s in sums):
            _slot(sums, lambda: ())
        feeds, attends = [s.result() for s in feeds], [s.result() for s in attends]
        grads = feeds + attends
        total = sum(jnp.sum(jnp.square(g.astype(F32))) for g in grads)
        count = sum(g.size for g in grads)
        factor = jnp.minimum(1.0, 0.5 * lax.rsqrt(total / count + 1e-30))
        return _adamw(factor.reshape(1), weights, m, v, feeds, attends)

    states, all_of = P(("rep", "dp"), None, None), P(None, None, None)
    return jax.shard_map(
        step,
        mesh=mesh,
        in_specs=(states, states) + (all_of,) * 21,
        out_specs=(P("rep", None, None),) * 21,
        check_vma=False,
    )
```

```python
import functools

import jax
import jax.numpy as jnp
from jax import lax
from jax.experimental import pallas as pl
from jax.experimental.pallas import tpu as pltpu
from jax.sharding import PartitionSpec as P

BF, F32 = jnp.bfloat16, jnp.float32
LOG2E = 1.4426950408889634
HEAD = 256
THETA = 10000
HALF = HEAD // 2
TILE = 512
FB = 512
VMEM = 60 * 2**20


def _dot(a, b, ca=1, cb=0):
    return lax.dot_general(a, b, (((ca,), (cb,)), ((), ())), preferred_element_type=F32)


def _norm(h):
    wide = h.astype(F32)
    scale = lax.rsqrt(jnp.mean(wide * wide, -1, keepdims=True) + 1e-6)
    return (wide * scale).astype(BF), wide, scale


def _norm_back(by_out, wide, scale):
    by_scale = jnp.sum(by_out * wide, -1, keepdims=True)
    return by_out * scale - wide * (by_scale * scale * scale * scale * (1.0 / wide.shape[-1]))


def _turn(t, cos, sin, back=False):
    a, b = t[:, :HALF].astype(F32), t[:, HALF:].astype(F32)
    if back:
        return jnp.concatenate([a * cos + b * sin, b * cos - a * sin], -1).astype(BF)
    return jnp.concatenate([a * cos - b * sin, b * cos + a * sin], -1).astype(BF)


def _params(semantics, **more):
    return pltpu.CompilerParams(dimension_semantics=semantics, vmem_limit_bytes=VMEM, **more)


def _cost(flops, bytes_, exps=0):
    return pl.CostEstimate(flops=int(flops), bytes_accessed=int(bytes_), transcendentals=int(exps))


def _qkv_kernel(h_ref, wq_ref, wk_ref, wv_ref, cos_ref, sin_ref, q_ref, k_ref, v_ref):
    a, _, _ = _norm(h_ref[...])
    cos, sin = cos_ref[...], sin_ref[...]
    for w_ref, out in ((wq_ref, q_ref), (wk_ref, k_ref)):
        t = _dot(a, w_ref[0]).astype(BF)
        for at in range(0, t.shape[1], HEAD):
            out[:, at : at + HEAD] = _turn(t[:, at : at + HEAD], cos, sin)
    v_ref[...] = _dot(a, wv_ref[0]).astype(BF)


def _qkv(h, wq, wk, wv, cos, sin, layer):
    t, d = h.shape
    rows = pl.BlockSpec((TILE, d), lambda i: (i, 0))
    whole = pl.BlockSpec((1, d, d), lambda i: (layer, 0, 0))
    table = pl.BlockSpec((TILE, HALF), lambda i: (i, 0))
    return pl.pallas_call(
        _qkv_kernel,
        grid=(t // TILE,),
        in_specs=[rows, whole, whole, whole, table, table],
        out_specs=[rows] * 3,
        out_shape=[jax.ShapeDtypeStruct((t, d), BF)] * 3,
        compiler_params=_params(("arbitrary",)),
        cost_estimate=_cost(6 * t * d * d, 8 * t * d + 6 * d * d),
        name="qkv",
    )(h, wq, wk, wv, cos, sin)


def _attend_kernel(q_ref, k_ref, v_ref, o_ref, lse_ref, vt_s, p_s):
    t = q_ref.shape[0]
    e = HEAD**-0.5 * LOG2E
    vt_s[...] = v_ref[...].T
    hide = lax.broadcasted_iota(jnp.int32, (TILE, TILE), 0) > lax.broadcasted_iota(jnp.int32, (TILE, TILE), 1)
    for at in range(0, t, TILE):
        q = q_ref[at : at + TILE, :]
        scores = [_dot(k_ref[j : j + TILE, :], q, 1, 1) for j in range(0, at + TILE, TILE)]
        scores[-1] = jnp.where(hide, -jnp.inf, scores[-1])
        top = functools.reduce(jnp.maximum, [s.max(axis=0, keepdims=True) for s in scores])
        total = 0.0
        for n, s in enumerate(scores):
            p = jnp.exp2((s - top) * e)
            total = total + p.sum(axis=0, keepdims=True)
            p_s[n * TILE : (n + 1) * TILE, :] = p.astype(BF)
        mix = _dot(vt_s[:, : at + TILE], p_s[: at + TILE, :])
        o_ref[at : at + TILE, :] = (mix * (1.0 / total)).T.astype(BF)
        lse_ref[0, :, at : at + TILE] = top * e + jnp.log2(total)


def _attend(q, k, v):
    t, d = q.shape
    head = pl.BlockSpec((t, HEAD), lambda h: (0, h))
    return pl.pallas_call(
        _attend_kernel,
        grid=(d // HEAD,),
        in_specs=[head] * 3,
        out_specs=[head, pl.BlockSpec((1, 1, t), lambda h: (h, 0, 0))],
        out_shape=[jax.ShapeDtypeStruct((t, d), BF), jax.ShapeDtypeStruct((d // HEAD, 1, t), F32)],
        scratch_shapes=[pltpu.VMEM((HEAD, t), BF), pltpu.VMEM((t, TILE), BF)],
        compiler_params=_params(("arbitrary",)),
        cost_estimate=_cost(2.5 * t * t * d, 8 * t * d, t * t),
        name="attend",
    )(q, k, v)


def _mix_kernel(h_ref, o_ref, wo_ref, h2_ref):
    h2_ref[...] = h_ref[...] + _dot(o_ref[...], wo_ref[0]).astype(BF)


def _mix(h, o, wo, layer):
    t, d = h.shape
    rows = pl.BlockSpec((TILE, d), lambda i: (i, 0))
    return pl.pallas_call(
        _mix_kernel,
        grid=(t // TILE,),
        in_specs=[rows, rows, pl.BlockSpec((1, d, d), lambda i: (layer, 0, 0))],
        out_specs=rows,
        out_shape=jax.ShapeDtypeStruct((t, d), BF),
        compiler_params=_params(("arbitrary",)),
        cost_estimate=_cost(2 * t * d * d, 6 * t * d),
        name="mix",
    )(h, o, wo)


def _feed_kernel(h_ref, o_ref, wo_ref, wg_ref, wu_ref, wd_ref, h2_ref, h3_ref):
    h2 = h_ref[...] + _dot(o_ref[...], wo_ref[0]).astype(BF)
    h2_ref[...] = h2
    b, _, _ = _norm(h2)
    out = 0.0
    for at in range(0, wg_ref.shape[2], FB):
        gate, up = _dot(b, wg_ref[0, :, at : at + FB]), _dot(b, wu_ref[0, :, at : at + FB])
        act = (gate * jax.nn.sigmoid(gate) * up).astype(BF)
        out = out + _dot(act, wd_ref[0, at : at + FB, :])
    h3_ref[...] = h2 + out.astype(BF)


def _feed(h, o, wo, wg, wu, wd, layer):
    t, d = h.shape
    f = wg.shape[2]
    rows = pl.BlockSpec((TILE, d), lambda i: (i, 0))
    whole = lambda *shape: pl.BlockSpec((1, *shape), lambda i: (layer, 0, 0))
    return pl.pallas_call(
        _feed_kernel,
        grid=(t // TILE,),
        in_specs=[rows, rows, whole(d, d), whole(d, f), whole(d, f), whole(f, d)],
        out_specs=[rows, rows],
        out_shape=[jax.ShapeDtypeStruct((t, d), BF)] * 2,
        compiler_params=_params(("arbitrary",)),
        cost_estimate=_cost(2 * t * d * d + 6 * t * d * f, 8 * t * d + 6 * d * f, t * f),
        name="feed",
    )(h, o, wo, wg, wu, wd)


FEEDS, HEADS = 4, 2
EACH = FEEDS + HEADS
PIECES = 2 * EACH
STAGES = 5
STEPS = PIECES + STAGES
HALFB = FB // 2
ROWS, LESS = 3 * HALFB, 2 * HALFB
BIG_VMEM = 67043328


def _is_feed(p):
    return ((p >= 0) & (p < FEEDS)) | ((p >= EACH) & (p < EACH + FEEDS))


def _is_head(p):
    return ((p >= FEEDS) & (p < EACH)) | ((p >= EACH + FEEDS) & (p < PIECES))


def _feed_step(first, last, wg_ref, wu_ref, wd_ref, term, h2_s, dh_s, b_s, bt_s, dht_s, db_s, dgate_s, dup_s, act_s):
    t = h2_s.shape[0]
    tiles = [slice(at, at + TILE) for at in range(0, t, TILE)]

    @pl.when(first)
    def _():
        for here in tiles:
            b, _, _ = _norm(h2_s[here, :])
            b_s[here, :] = b
            bt_s[:, here] = b.T
            dht_s[:, here] = dh_s[here, :].T
            db_s[here, :] = jnp.zeros_like(db_s[here, :])

    wg, wu, wd = wg_ref[0], wu_ref[0], wd_ref[0]
    for here in tiles:
        b = b_s[here, :]
        gate, up = _dot(b, wg), _dot(b, wu)
        dact = _dot(dh_s[here, :], wd, 1, 1).astype(BF).astype(F32)
        sig = jax.nn.sigmoid(gate)
        silu = gate * sig
        act_s[here, :] = (silu * up).astype(BF)
        dup = (dact * silu).astype(BF)
        dgate = (dact * up * (sig + silu * (1.0 - sig))).astype(BF)
        dup_s[here, :] = dup
        dgate_s[here, :] = dgate
        db_s[here, :] += _dot(dgate, wg, 1, 1) + _dot(dup, wu, 1, 1)
    for m, dw in enumerate((_dot(bt_s[...], dgate_s[...]), _dot(bt_s[...], dup_s[...]), _dot(dht_s[...], act_s[...]).T)):
        dw = dw.astype(BF)
        term[0, m * HALFB : (m + 1) * HALFB, :] = dw[:HALFB, :]
        term[1, m * HALFB : (m + 1) * HALFB, :] = dw[HALFB:, :]

    @pl.when(last)
    def _():
        for here in tiles:
            _, wide, scale = _norm(h2_s[here, :])
            dh_s[here, :] = dh_s[here, :] + _norm_back(db_s[here, :], wide, scale).astype(BF)


def _head_step(first, last, with_dh, wo_ref, wq_ref, wk_ref, wv_ref, cos_ref, sin_ref, lse_ref, term, q_ref, k_ref, v_ref, o_ref, h_s, dh_s, at_s, da_s,
               do_s, dqt_s):
    t = h_s.shape[0]
    scale = HEAD**-0.5
    e = scale * LOG2E
    tiles = [slice(at, at + TILE) for at in range(0, t, TILE)]

    def put(m, half, x):
        term[half, (m // 2) * HEAD : (m // 2 + 1) * HEAD, (m % 2) * HEAD : (m % 2 + 1) * HEAD] = x

    @pl.when(first)
    def _():
        for here in tiles:
            at_s[:, here] = _norm(h_s[here, :])[0].T
            da_s[here, :] = jnp.zeros_like(da_s[here, :])

    deltas = []
    for here in tiles:
        do = _dot(dh_s[here, :], wo_ref[0], 1, 1).astype(BF)
        do_s[here, :HEAD] = do
        both = do.astype(F32) * o_ref[here, :].astype(F32)
        deltas.append((both[:, :HALF] + both[:, HALF:]).T.sum(axis=0, keepdims=True))
    delta = jnp.concatenate(deltas, axis=1)
    dwo = _dot(o_ref[...].T, dh_s[...]).astype(BF)
    put(3, 0, dwo[:, :HEAD])
    put(3, 1, dwo[:, HEAD:])

    hide = lax.broadcasted_iota(jnp.int32, (TILE, TILE), 0) > lax.broadcasted_iota(jnp.int32, (TILE, TILE), 1)
    dks, dvs = [], []
    for at in range(0, t, TILE):
        k, v = k_ref[at : at + TILE, :], v_ref[at : at + TILE, :]
        kt = k.T
        ps, dss = [], []
        for i in range(at, t, TILE):
            here = slice(i, i + TILE)
            p = jnp.exp2(_dot(k, q_ref[here, :], 1, 1) * e - lse_ref[:, here])
            if i == at:
                p = jnp.where(hide, 0.0, p)
            ds = (p * (_dot(v, do_s[here, :HEAD], 1, 1) - delta[:, here])).astype(BF)
            ps.append(p.astype(BF))
            dss.append(ds)
        p, ds = jnp.concatenate(ps, axis=1), jnp.concatenate(dss, axis=1)
        dvs.append(_dot(p, do_s[at:, :HEAD]).astype(BF))
        dks.append((_dot(ds, q_ref[at:, :]) * scale).astype(BF))
        dq = _dot(kt, ds)
        dqt_s[:, at:] = dq if at == 0 else dqt_s[:, at:] + dq

    for m, w_ref in enumerate((wq_ref, wk_ref, wv_ref)):
        parts = []
        for j, here in enumerate(tiles):
            part = (dqt_s[:, here] * scale).T.astype(BF) if m == 0 else (dks, dvs)[m - 1][j]
            parts.append(_turn(part, cos_ref[here, :], sin_ref[here, :], True) if m < 2 else part)
        part = jnp.concatenate(parts, axis=0)
        dw = _dot(at_s[...], part).astype(BF)
        put(m, 0, dw[:HEAD, :])
        put(m, 1, dw[HEAD:, :])

        @pl.when(with_dh)
        def _():
            da_s[...] += _dot(part, w_ref[0], 1, 1)

    @pl.when(with_dh & last)
    def _():
        for here in tiles:
            _, wide, s = _norm(h_s[here, :])
            dh_s[here, :] = dh_s[here, :] + _norm_back(da_s[here, :], wide, s).astype(BF)


def _backward_kernel(count, *refs):
    (dy, h2s, hs, qkvo, lses) = refs[0], refs[1:3], refs[3:5], (refs[5:9], refs[9:13]), refs[13:15]
    wg_ref, wu_ref, wd_ref, wo_ref, wq_ref, wk_ref, wv_ref, cos_ref, sin_ref = refs[15:24]
    out_ref, factor_ref = refs[24:26]
    (h2_s, dh_s, h_s, qkvo_s, b_s, bt_s, dht_s, db_s, dgate_s, dup_s, act_s, dqt_s,
     term, swapped, both, wide_both, inward, side, received, total, mine, other, squares,
     load_sem, send_sem, recv_sem, from_partner, from_inner, from_outer) = refs[26:]
    s = pl.program_id(0)
    par = lax.rem(s, 2)
    me = lax.axis_index("dp")
    core, chip = lax.rem(me, 2), lax.div(me, 2)
    partner = me + 1 - 2 * core
    end = (chip == 0) | (chip == 3)
    middle = (chip == 1) | (chip == 2)
    inner = jnp.where(chip < 2, me + 2, me - 2)
    outer = jnp.where(chip == 1, me - 2, jnp.where(chip == 2, me + 2, inner))

    def tell(semaphore, device):
        pl.semaphore_signal(semaphore, inc=1, device_id={"dp": device}, device_id_type=pl.DeviceIdType.MESH)

    def load(n, src, dst):
        return pltpu.make_async_copy(src, dst, load_sem.at[n])

    def heads(layer):
        cs = [load(1 + 4 * n + i, qkvo[layer][i].at[:, n * HEAD : (n + 1) * HEAD], qkvo_s.at[n, i]) for n in range(HEADS) for i in range(4)]
        return [load(0, hs[layer], h_s), *cs]

    def opening():
        return [load(9, h2s[1], h2_s), load(10, dy, dh_s)]

    @pl.when(s == 0)
    def _():
        for c in opening() + heads(1):
            c.start()
        barrier = pltpu.get_barrier_semaphore()
        tell(barrier, partner)
        tell(barrier, inner)

        @pl.when(middle)
        def _():
            tell(barrier, outer)
            pl.semaphore_wait(barrier, 3)

        @pl.when(end)
        def _():
            pl.semaphore_wait(barrier, 2)

        squares[...] = jnp.zeros_like(squares)
        for c in opening():
            c.wait()

    @pl.when(s == FEEDS)
    def _():
        for c in heads(1):
            c.wait()
        load(9, h2s[0], h2_s).start()

    @pl.when(s == EACH)
    def _():
        load(9, h2s[0], h2_s).wait()
        for c in heads(0):
            c.start()

    @pl.when(s == EACH + FEEDS)
    def _():
        for c in heads(0):
            c.wait()

    @pl.when(s >= 2)
    def _():
        pl.semaphore_wait(from_partner, 1)
        pl.semaphore_wait(from_inner, 1)

        @pl.when(middle)
        def _():
            pl.semaphore_wait(from_outer, 1)

    def copy(stage, rows):
        src = (term.at[1 - par, 1 - core], both, side, total, mine)[stage]
        dst = (swapped, inward, received, received, other)[stage].at[par]
        to = (partner, inner, inner, outer, partner)[stage]
        return pltpu.make_async_remote_copy(
            src_ref=src.at[0:rows], dst_ref=dst.at[0:rows], send_sem=send_sem.at[stage, par], recv_sem=recv_sem.at[stage, par],
            device_id={"dp": to}, device_id_type=pl.DeviceIdType.MESH)

    who_sends = (None, end, middle, middle, None)
    who_gets = (None, middle, middle, end, None)

    def on(who, stage, what):
        p = s - 1 - stage
        for kind, rows in ((_is_feed(p), ROWS), (_is_head(p), LESS)):
            pl.when(kind if who is None else kind & who)(functools.partial(what, rows))

    for stage in range(STAGES):
        on(who_sends[stage], stage, lambda rows, stage=stage: copy(stage, rows).start())

    mine_now = term.at[par]

    @pl.when(_is_feed(s))
    def _():
        _feed_step((s == 0) | (s == EACH), (s == FEEDS - 1) | (s == EACH + FEEDS - 1), wg_ref, wu_ref, wd_ref, mine_now, h2_s, dh_s, b_s, bt_s, dht_s,
                   db_s, dgate_s, dup_s, act_s)

    @pl.when(_is_head(s))
    def _():
        upper = s < EACH
        n = jnp.where(upper, s - FEEDS, s - EACH - FEEDS)
        lse = jnp.where(upper, lses[1][n], lses[0][n])
        _head_step(n == 0, n == HEADS - 1, upper, wo_ref, wq_ref, wk_ref, wv_ref, cos_ref, sin_ref, lse, mine_now, *(qkvo_s.at[n, i] for i in range(4)),
                   h_s, dh_s, bt_s, db_s, dup_s, dqt_s)

    def squared(x):
        x = x.astype(F32)
        return jnp.sum((x * x).reshape(-1, 8, FB), axis=0)

    def wait(stage):
        on(who_sends[stage], stage, lambda rows: copy(stage, rows).wait_send())
        on(who_gets[stage], stage, lambda rows: copy(stage, rows).wait_recv())

    def take(who, stage, what):
        p = s - 1 - stage
        there = (p >= 0) & (p < PIECES)
        pl.when(there if who is None else there & who)(what)

    wait(4)

    def keep(rows):
        out_ref[0, core] = mine[...]
        out_ref[0, 1 - core] = other[par]
        squares[0] += squared(mine[:rows, :])
        squares[1] += squared(other[par, :rows, :])

    on(None, 4, keep)
    wait(3)

    def settle_middle():
        mine[...] = total[...]

    def settle_end():
        mine[...] = received[par]

    take(middle, 3, settle_middle)
    take(end, 3, settle_end)
    wait(2)

    def join_across():
        total[...] = (side[...].astype(F32) + received[par].astype(F32)).astype(BF)

    take(middle, 2, join_across)
    wait(1)

    def join_inward():
        side[...] = (wide_both[...] + inward[par].astype(F32)).astype(BF)

    take(middle, 1, join_inward)
    wait(0)

    def join_cores_end():
        both[...] = (term[1 - par, core].astype(F32) + swapped[par].astype(F32)).astype(BF)

    def join_cores_middle():
        wide_both[...] = term[1 - par, core].astype(F32) + swapped[par].astype(F32)

    take(end, 0, join_cores_end)
    take(middle, 0, join_cores_middle)

    @pl.when(s < STEPS - 2)
    def _():
        tell(from_partner, partner)

        @pl.when(end)
        def _():
            tell(from_outer, inner)

        @pl.when(middle)
        def _():
            tell(from_inner, inner)
            tell(from_inner, outer)

    @pl.when(s == STEPS - 1)
    def _():
        both_halves = jnp.sum(squares[0], keepdims=True) + jnp.sum(squares[1], keepdims=True)
        factor = jnp.minimum(1.0, 0.5 * lax.rsqrt(both_halves * (1.0 / count) + 1e-30))
        factor_ref[...] = jnp.broadcast_to(factor, factor_ref.shape)


def _backward(dy, kept, weights, cos, sin):
    wq, wk, wv, wo, wg, wu, wd = weights
    t, d = dy.shape
    count = sum(w.size for w in weights)

    def feed_at(s):
        return jnp.where(s < EACH, 1, 0), jnp.minimum(jnp.where(s < EACH, s, s - EACH), FEEDS - 1)

    def head_at(s):
        return jnp.where(s < EACH, 1, 0), jnp.clip(jnp.where(s < EACH, s - FEEDS, s - EACH - FEEDS), 0, HEADS - 1)

    def across(s):
        layer, n = feed_at(s)
        return layer, 0, n

    def down(s):
        layer, n = feed_at(s)
        return layer, n, 0

    def head_across(s):
        layer, n = head_at(s)
        return layer, 0, n

    def head_down(s):
        layer, n = head_at(s)
        return layer, n, 0

    hbm = pl.BlockSpec(memory_space=pltpu.HBM)
    fixed = lambda a: pl.BlockSpec(a.shape, lambda s: (0,) * a.ndim, pipeline_mode=pl.Buffered(1))
    given = [dy, *(k[6] for k in kept), *(k[0] for k in kept), *kept[0][1:5], *kept[1][1:5], *(k[5] for k in kept)]
    specs = [hbm] * 13 + [fixed(k[5]) for k in kept]
    given += [wg, wu, wd, wo, wq, wk, wv, cos, sin]
    specs += [pl.BlockSpec((1, d, FB), across)] * 2 + [pl.BlockSpec((1, FB, d), down), pl.BlockSpec((1, HEAD, d), head_down)]
    specs += [pl.BlockSpec((1, d, HEAD), head_across)] * 3 + [fixed(cos), fixed(sin)]
    tokens = pltpu.VMEM((t, d), BF)
    half = pltpu.VMEM((ROWS, FB), BF)
    halves = pltpu.VMEM((2, ROWS, FB), BF)
    return pl.pallas_call(
        functools.partial(_backward_kernel, count),
        grid=(STEPS,),
        in_specs=specs,
        out_specs=[pl.BlockSpec((1, 2, ROWS, FB), lambda s: (jnp.clip(s - STAGES, 0, PIECES - 1), 0, 0, 0)), pl.BlockSpec((8, 128), lambda s: (0, 0))],
        out_shape=[jax.ShapeDtypeStruct((PIECES, 2, ROWS, FB), BF), jax.ShapeDtypeStruct((8, 128), F32)],
        scratch_shapes=[tokens, tokens, tokens, pltpu.VMEM((HEADS, 4, t, HEAD), BF), tokens, pltpu.VMEM((d, t), BF), pltpu.VMEM((d, t), BF),
                        pltpu.VMEM((t, d), F32), pltpu.VMEM((t, FB), BF), pltpu.VMEM((t, FB), BF), pltpu.VMEM((t, FB), BF), pltpu.VMEM((HEAD, t), F32),
                        pltpu.VMEM((2, 2, ROWS, FB), BF), halves, half, pltpu.VMEM((ROWS, FB), F32), halves, half, halves, half, half, halves,
                        pltpu.VMEM((2, 8, FB), F32),
                        pltpu.SemaphoreType.DMA((11,)), pltpu.SemaphoreType.DMA((STAGES, 2)), pltpu.SemaphoreType.DMA((STAGES, 2)),
                        pltpu.SemaphoreType.REGULAR, pltpu.SemaphoreType.REGULAR, pltpu.SemaphoreType.REGULAR],
        compiler_params=pltpu.CompilerParams(dimension_semantics=("arbitrary",), vmem_limit_bytes=BIG_VMEM, collective_id=0, has_side_effects=True),
        cost_estimate=_cost(2 * (16 * t * d * 2048 + 12 * t * t * d + 16 * t * d * d), 60 * t * d),
        name="backward",
    )(*given)


def _adamw_kernel(*refs):
    w_refs, m_refs, v_refs, feed_ref, head_ref, factor_ref, outs = refs[:7], refs[7:14], refs[14:21], refs[21], refs[22], refs[23], refs[24:]
    factor = factor_ref[0:1, 0:1]

    def one(i, g):
        g = g.astype(F32) * factor
        m = 0.9 * m_refs[i][0] + 0.1 * g
        v = 0.95 * v_refs[i][0] + 0.05 * g * g
        w = w_refs[i][0].astype(F32)
        outs[i][0] = (w - 0.02 * (m * lax.rsqrt(v + 1e-8) + 0.1 * w)).astype(BF)
        outs[7 + i][0] = m
        outs[14 + i][0] = v

    for i in range(4):
        one(i, head_ref[0, 0, i // 2, 0, :, (i % 2) * HEAD : (i % 2 + 1) * HEAD])
    for i in range(3):
        one(4 + i, feed_ref[0, 0, i].reshape(HALFB, FB))


def _adamw(factor, weights, m, v, pieces):
    layers = weights[0].shape[0]
    thin = HEAD // 2
    by_rows = pl.BlockSpec((1, thin, HEAD), lambda l, f, r: (l, (f % 2) * 2 + r, f // 2))
    by_columns = pl.BlockSpec((1, thin, HEAD), lambda l, f, r: (l, (f // 2) * 2 + r, f % 2))
    wide = pl.BlockSpec((1, HALFB, FB), lambda l, f, r: (l, r, f))
    down = pl.BlockSpec((1, HALFB, FB), lambda l, f, r: (l, 2 * f + r, 0))
    like = [by_rows, by_rows, by_rows, by_columns, wide, wide, down]
    pieces = pieces.reshape(PIECES, 2, 3, 2, thin, FB)
    feed = pl.BlockSpec((1, 1, 3, 2, thin, FB), lambda l, f, r: ((1 - l) * EACH + f, r, 0, 0, 0, 0))
    head = pl.BlockSpec((1, 1, 3, 1, thin, FB), lambda l, f, r: ((1 - l) * EACH + FEEDS + f // 2, f % 2, 0, r, 0, 0))
    return pl.pallas_call(
        _adamw_kernel,
        grid=(layers, FEEDS, 2),
        in_specs=like * 3 + [feed, head, pl.BlockSpec((8, 128), lambda l, f, r: (0, 0))],
        out_specs=like * 3,
        out_shape=[jax.ShapeDtypeStruct(w.shape, BF) for w in weights] + [jax.ShapeDtypeStruct(w.shape, F32) for w in weights] * 2,
        compiler_params=_params(("arbitrary",) * 3),
        cost_estimate=_cost(200 * 2**20, 180 * 2**20),
        name="adamw",
    )(*weights, *m, *v, pieces, pieces, factor)


def solution(mesh):
    def step(x, dy, *arrays):
        weights, m, v = (arrays[i : i + 7] for i in (0, 7, 14))
        wq, wk, wv, wo, wg, wu, wd = weights
        layers = wq.shape[0]
        h, t = x[0], x.shape[1]
        angle = jnp.arange(t, dtype=F32)[:, None] * THETA ** (-jnp.arange(HALF, dtype=F32) / HALF)
        cos, sin = jnp.cos(angle), jnp.sin(angle)
        kept = []
        for n in range(layers):
            q, k, val = _qkv(h, wq, wk, wv, cos, sin, n)
            o, lse = _attend(q, k, val)
            if n < layers - 1:
                h2, h3 = _feed(h, o, wo, wg, wu, wd, n)
            else:
                h2, h3 = _mix(h, o, wo, n), None
            kept.append((h, q, k, val, o, lse, h2))
            h = h3
        pieces, factor = _backward(dy[0], kept, weights, cos, sin)
        return tuple(_adamw(factor, weights, m, v, pieces))

    states, all_of = P(("rep", "dp"), None, None), P(None, None, None)
    return jax.shard_map(
        step,
        mesh=mesh,
        in_specs=(states, states) + (all_of,) * 21,
        out_specs=(P("rep", None, None),) * 21,
        check_vma=False,
    )
```

```python
import functools

import jax
import jax.numpy as jnp
import numpy as np
from jax import lax
from jax.experimental import pallas as pl
from jax.experimental.pallas import tpu as pltpu
from jax.sharding import PartitionSpec as P

BF, F32 = jnp.bfloat16, jnp.float32
LOG2E = 1.4426950408889634
HEAD = 256
THETA = 10000
HALF = HEAD // 2
TILE = 512
FINE = 64
FB = 512
VMEM = 60 * 2**20


def _dot(a, b, ca=1, cb=0):
    return lax.dot_general(a, b, (((ca,), (cb,)), ((), ())), preferred_element_type=F32)


def _norm(h):
    wide = h.astype(F32)
    scale = lax.rsqrt(jnp.mean(wide * wide, -1, keepdims=True) + 1e-6)
    return (wide * scale).astype(BF), wide, scale


def _norm_back(by_out, wide, scale):
    by_scale = jnp.sum(by_out * wide, -1, keepdims=True)
    return by_out * scale - wide * (by_scale * scale * scale * scale * (1.0 / wide.shape[-1]))


def _turn(t, cos, sin, back=False):
    a, b = t[:, :HALF].astype(F32), t[:, HALF:].astype(F32)
    if back:
        return jnp.concatenate([a * cos + b * sin, b * cos - a * sin], -1).astype(BF)
    return jnp.concatenate([a * cos - b * sin, b * cos + a * sin], -1).astype(BF)


def _params(semantics, **more):
    return pltpu.CompilerParams(dimension_semantics=semantics, vmem_limit_bytes=VMEM, **more)


def _cost(flops, bytes_, exps=0):
    return pl.CostEstimate(flops=int(flops), bytes_accessed=int(bytes_), transcendentals=int(exps))


def _tables(t):
    rate = THETA ** (-np.arange(HALF) / HALF)
    far, near = np.arange(0, t, FINE)[:, None] * rate, np.arange(FINE)[:, None] * rate
    return tuple(jnp.asarray(x, F32) for x in (np.cos(far), np.sin(far), np.cos(near), np.sin(near)))


def _spread(tables, cos_ref, sin_ref, first, count):
    cos_far, sin_far, cos_near, sin_near = tables
    c, s = cos_near[...], sin_near[...]
    for i in range(count // FINE):
        here = pl.ds(first // FINE + i, 1) if isinstance(first, int) else pl.ds(lax.div(first, FINE) + i, 1)
        cf, sf = cos_far[here, :], sin_far[here, :]
        cos_ref[i * FINE : (i + 1) * FINE, :] = cf * c - sf * s
        sin_ref[i * FINE : (i + 1) * FINE, :] = sf * c + cf * s


def _qkv_kernel(h_ref, wq_ref, wk_ref, wv_ref, *refs):
    tables, (q_ref, k_ref, v_ref, cos_ref, sin_ref) = refs[:4], refs[4:]
    a, _, _ = _norm(h_ref[...])
    _spread(tables, cos_ref, sin_ref, pl.program_id(0) * TILE, TILE)
    cos, sin = cos_ref[...], sin_ref[...]
    for w_ref, out in ((wq_ref, q_ref), (wk_ref, k_ref)):
        t = _dot(a, w_ref[0]).astype(BF)
        for at in range(0, t.shape[1], HEAD):
            out[:, at : at + HEAD] = _turn(t[:, at : at + HEAD], cos, sin)
    v_ref[...] = _dot(a, wv_ref[0]).astype(BF)


def _qkv(h, wq, wk, wv, tables, layer):
    t, d = h.shape
    rows = pl.BlockSpec((TILE, d), lambda i: (i, 0))
    whole = pl.BlockSpec((1, d, d), lambda i: (layer, 0, 0))
    tabled = [pl.BlockSpec(a.shape, lambda i: (0, 0)) for a in tables]
    return pl.pallas_call(
        _qkv_kernel,
        grid=(t // TILE,),
        in_specs=[rows, whole, whole, whole, *tabled],
        out_specs=[rows] * 3,
        out_shape=[jax.ShapeDtypeStruct((t, d), BF)] * 3,
        scratch_shapes=[pltpu.VMEM((TILE, HALF), F32)] * 2,
        compiler_params=_params(("arbitrary",)),
        cost_estimate=_cost(6 * t * d * d, 8 * t * d + 6 * d * d),
        name="qkv",
    )(h, wq, wk, wv, *tables)


def _attend_kernel(q_ref, k_ref, v_ref, o_ref, lse_ref, vt_s, p_s):
    t = q_ref.shape[0]
    e = HEAD**-0.5 * LOG2E
    vt_s[...] = v_ref[...].T
    hide = lax.broadcasted_iota(jnp.int32, (TILE, TILE), 0) > lax.broadcasted_iota(jnp.int32, (TILE, TILE), 1)
    for at in range(0, t, TILE):
        q = q_ref[at : at + TILE, :]
        scores = [_dot(k_ref[j : j + TILE, :], q, 1, 1) for j in range(0, at + TILE, TILE)]
        scores[-1] = jnp.where(hide, -jnp.inf, scores[-1])
        top = functools.reduce(jnp.maximum, [s.max(axis=0, keepdims=True) for s in scores])
        total = 0.0
        for n, s in enumerate(scores):
            p = jnp.exp2((s - top) * e)
            total = total + p.sum(axis=0, keepdims=True)
            p_s[n * TILE : (n + 1) * TILE, :] = p.astype(BF)
        mix = _dot(vt_s[:, : at + TILE], p_s[: at + TILE, :])
        o_ref[at : at + TILE, :] = (mix * (1.0 / total)).T.astype(BF)
        lse_ref[0, :, at : at + TILE] = top * e + jnp.log2(total)


def _attend(q, k, v):
    t, d = q.shape
    head = pl.BlockSpec((t, HEAD), lambda h: (0, h))
    return pl.pallas_call(
        _attend_kernel,
        grid=(d // HEAD,),
        in_specs=[head] * 3,
        out_specs=[head, pl.BlockSpec((1, 1, t), lambda h: (h, 0, 0))],
        out_shape=[jax.ShapeDtypeStruct((t, d), BF), jax.ShapeDtypeStruct((d // HEAD, 1, t), F32)],
        scratch_shapes=[pltpu.VMEM((HEAD, t), BF), pltpu.VMEM((t, TILE), BF)],
        compiler_params=_params(("arbitrary",)),
        cost_estimate=_cost(2.5 * t * t * d, 8 * t * d, t * t),
        name="attend",
    )(q, k, v)


def _feed_kernel(h_ref, o_ref, wo_ref, wg_ref, wu_ref, wd_ref, h2_ref, h3_ref):
    h2 = h_ref[...] + _dot(o_ref[...], wo_ref[0]).astype(BF)
    h2_ref[...] = h2
    b, _, _ = _norm(h2)
    out = 0.0
    for at in range(0, wg_ref.shape[2], FB):
        gate, up = _dot(b, wg_ref[0, :, at : at + FB]), _dot(b, wu_ref[0, :, at : at + FB])
        act = (gate * (0.5 * jnp.tanh(0.5 * gate) + 0.5) * up).astype(BF)
        out = out + _dot(act, wd_ref[0, at : at + FB, :])
    h3_ref[...] = h2 + out.astype(BF)


def _feed(h, o, wo, wg, wu, wd, layer):
    t, d = h.shape
    f = wg.shape[2]
    rows = pl.BlockSpec((TILE, d), lambda i: (i, 0))
    whole = lambda *shape: pl.BlockSpec((1, *shape), lambda i: (layer, 0, 0))
    return pl.pallas_call(
        _feed_kernel,
        grid=(t // TILE,),
        in_specs=[rows, rows, whole(d, d), whole(d, f), whole(d, f), whole(f, d)],
        out_specs=[rows, rows],
        out_shape=[jax.ShapeDtypeStruct((t, d), BF)] * 2,
        compiler_params=_params(("arbitrary",)),
        cost_estimate=_cost(2 * t * d * d + 6 * t * d * f, 8 * t * d + 6 * d * f, t * f),
        name="feed",
    )(h, o, wo, wg, wu, wd)


FEEDS, HEADS = 4, 2
EACH = FEEDS + HEADS
PIECES = 2 * EACH
FEED_UNITS, HEAD_UNITS = 3, 2
LAYER_UNITS = FEEDS * FEED_UNITS + HEADS * HEAD_UNITS
UNITS = 2 * LAYER_UNITS
FIRST = 3
STARTS = (0, 1, 3, 5, 7, 9, 10)
STAGES = 5
SLOTS = 4
RING = 6
LAST = UNITS - 1 + FIRST + STARTS[-1]
STEPS = PIECES + (LAST + 1 - UNITS + 2) // 3
HALFB = FB // 2
BIG_VMEM = 67043328


def _first_tick(s):
    layer = lax.div(s, EACH)
    return jnp.where(s < PIECES, layer * LAYER_UNITS + lax.div(5 * (s - layer * EACH) + 1, 2), UNITS + 3 * (s - PIECES))


def _has_tick(s, j):
    if j == 0:
        return s >= 0
    usual = _first_tick(s) + j <= LAST
    if j == 1:
        return usual
    r = lax.rem(s, EACH)
    return usual & ((s >= PIECES) | ((r != 1) & (r != 3)))


def _first_unit(s):
    layer = lax.div(s, EACH)
    r = s - layer * EACH
    return layer * LAYER_UNITS + jnp.where(r < FEEDS, FEED_UNITS * r, FEEDS * FEED_UNITS + HEAD_UNITS * (r - FEEDS))


def _is_feed(p):
    return ((p >= 0) & (p < FEEDS)) | ((p >= EACH) & (p < EACH + FEEDS))


def _is_head(p):
    return ((p >= FEEDS) & (p < EACH)) | ((p >= EACH + FEEDS) & (p < PIECES))


def _feed_parts(first, last, wg_ref, wu_ref, wd_ref, term, h2_s, dh_s, b_s, bt_s, dht_s, db_s, dgate_s, dup_s, act_s):
    t = h2_s.shape[0]
    tiles = [slice(at, at + TILE) for at in range(0, t, TILE)]

    def run(some):
        wg, wu, wd = wg_ref[0], wu_ref[0], wd_ref[0]
        for here in some:
            b = b_s[here, :]
            gate, up = _dot(b, wg), _dot(b, wu)
            dact = _dot(dh_s[here, :], wd, 1, 1).astype(BF).astype(F32)
            sig = 0.5 * jnp.tanh(0.5 * gate) + 0.5
            silu = gate * sig
            act_s[here, :] = (silu * up).astype(BF)
            dup = (dact * silu).astype(BF)
            dgate = (dact * up * (sig + silu * (1.0 - sig))).astype(BF)
            dup_s[here, :] = dup
            dgate_s[here, :] = dgate
            db_s[here, :] += _dot(dgate, wg, 1, 1) + _dot(dup, wu, 1, 1)

    def one():
        @pl.when(first)
        def _():
            for here in tiles:
                b, _, _ = _norm(h2_s[here, :])
                b_s[here, :] = b
                bt_s[:, here] = b.T
                dht_s[:, here] = dh_s[here, :].T
                db_s[here, :] = jnp.zeros_like(db_s[here, :])

        run(tiles[: len(tiles) // 2])

    def two():
        run(tiles[len(tiles) // 2 :])

    def three():
        for m, dw in enumerate((_dot(bt_s[...], dgate_s[...]), _dot(bt_s[...], dup_s[...]), _dot(dht_s[...], act_s[...]).T)):
            dw = dw.astype(BF)
            term(m)[0] = dw[:HALFB, :]
            term(m)[1] = dw[HALFB:, :]

        @pl.when(last)
        def _():
            for here in tiles:
                _, wide, scale = _norm(h2_s[here, :])
                dh_s[here, :] = dh_s[here, :] + _norm_back(db_s[here, :], wide, scale).astype(BF)

    return one, two, three


def _head_parts(first, last, with_dh, wo_ref, wq_ref, wk_ref, wv_ref, cos_ref, sin_ref, lse, term, q_ref, k_ref, v_ref, o_ref, h_s, dh_s, at_s, da_s,
                do_s, dkv_s, dqt_s, delta_s):
    t = h_s.shape[0]
    scale = HEAD**-0.5
    e = scale * LOG2E
    tiles = [slice(at, at + TILE) for at in range(0, t, TILE)]

    def put(m, half, x):
        term(m // 2)[half, :, (m % 2) * HEAD : (m % 2 + 1) * HEAD] = x

    def run(some):
        hide = lax.broadcasted_iota(jnp.int32, (TILE, TILE), 0) > lax.broadcasted_iota(jnp.int32, (TILE, TILE), 1)
        for tile in some:
            at = tile.start
            k, v = k_ref[tile, :], v_ref[tile, :]
            kt = k.T
            ps, dss = [], []
            for i in range(at, t, TILE):
                here = slice(i, i + TILE)
                p = jnp.exp2(_dot(k, q_ref[here, :], 1, 1) * e - lse[:, here])
                if i == at:
                    p = jnp.where(hide, 0.0, p)
                ds = (p * (_dot(v, do_s[here, :HEAD], 1, 1) - delta_s[:, here])).astype(BF)
                ps.append(p.astype(BF))
                dss.append(ds)
            p, ds = jnp.concatenate(ps, axis=1), jnp.concatenate(dss, axis=1)
            dkv_s[tile, :HEAD] = (_dot(ds, q_ref[at:, :]) * scale).astype(BF)
            dkv_s[tile, HEAD:] = _dot(p, do_s[at:, :HEAD]).astype(BF)
            dq = _dot(kt, ds)
            dqt_s[:, at:] = dq if at == 0 else dqt_s[:, at:] + dq

    def one():
        @pl.when(first)
        def _():
            for here in tiles:
                at_s[:, here] = _norm(h_s[here, :])[0].T
                da_s[here, :] = jnp.zeros_like(da_s[here, :])

        for here in tiles:
            do = _dot(dh_s[here, :], wo_ref[0], 1, 1).astype(BF)
            do_s[here, :HEAD] = do
            both = do.astype(F32) * o_ref[here, :].astype(F32)
            delta_s[:, here] = (both[:, :HALF] + both[:, HALF:]).T.sum(axis=0, keepdims=True)
        run(tiles[:1])

    def two():
        run(tiles[1:])

    def three():
        dwo = _dot(o_ref[...].T, dh_s[...]).astype(BF)
        put(3, 0, dwo[:, :HEAD])
        put(3, 1, dwo[:, HEAD:])
        for m, w_ref in enumerate((wq_ref, wk_ref, wv_ref)):
            parts = []
            for here in tiles:
                part = (dqt_s[:, here] * scale).T.astype(BF) if m == 0 else dkv_s[here, (m - 1) * HEAD : m * HEAD]
                parts.append(_turn(part, cos_ref[here, :], sin_ref[here, :], True) if m < 2 else part)
            part = jnp.concatenate(parts, axis=0)
            dw = _dot(at_s[...], part).astype(BF)
            put(m, 0, dw[:HEAD, :])
            put(m, 1, dw[HEAD:, :])

            @pl.when(with_dh)
            def _():
                da_s[...] += _dot(part, w_ref[0], 1, 1)

        @pl.when(with_dh & last)
        def _():
            for here in tiles:
                _, wide, s = _norm(h_s[here, :])
                dh_s[here, :] = dh_s[here, :] + _norm_back(da_s[here, :], wide, s).astype(BF)

    return one, two, three


def _backward_kernel(count, *refs):
    (dy, h2_low, hs, qkvo, lses) = refs[0], refs[1], refs[2:4], (refs[4:8], refs[8:12]), refs[12:14]
    wg_ref, wu_ref, wd_ref, wo_ref, wq_ref, wk_ref, wv_ref, wo_whole = refs[14:22]
    tables, out_ref, factor_ref = refs[22:26], refs[26], refs[27]
    (cos_ref, sin_ref, h2_s, dh_s, h_s, qkvo_s, b_s, bt_s, dht_s, db_s, dgate_s, dup_s, act_s, dqt_s, delta_s,
     term, swapped, both, wide_both, inward, side, received, total, mine, other, squares,
     load_sem, send_sem, recv_sem, write_sem, from_partner, from_inner, from_outer) = refs[28:]
    s = pl.program_id(0)
    me = lax.axis_index("dp")
    core, chip = lax.rem(me, 2), lax.div(me, 2)
    partner = me + 1 - 2 * core
    end = (chip == 0) | (chip == 3)
    middle = (chip == 1) | (chip == 2)
    inner = jnp.where(chip < 2, me + 2, me - 2)
    outer = jnp.where(chip == 1, me - 2, jnp.where(chip == 2, me + 2, inner))

    def tell(semaphore, device):
        pl.semaphore_signal(semaphore, inc=1, device_id={"dp": device}, device_id_type=pl.DeviceIdType.MESH)

    def load(n, src, dst):
        return pltpu.make_async_copy(src, dst, load_sem.at[n])

    def heads(layer, which):
        return [load(1 + 4 * n + i, qkvo[layer][i].at[:, n * HEAD : (n + 1) * HEAD], qkvo_s.at[n, i]) for n in range(HEADS) for i in which]

    @pl.when(s == 0)
    def _():
        dy_load = load(9, dy, dh_s)
        first_loads = [load(0, hs[1], h_s), *heads(1, (3,))]
        for c in [*first_loads, dy_load, *heads(1, (0, 1, 2))]:
            c.start()
        barrier = pltpu.get_barrier_semaphore()
        tell(barrier, partner)
        tell(barrier, inner)

        @pl.when(middle)
        def _():
            tell(barrier, outer)
            pl.semaphore_wait(barrier, 3)

        @pl.when(end)
        def _():
            pl.semaphore_wait(barrier, 2)

        squares[...] = jnp.zeros_like(squares)
        _spread(tables, cos_ref, sin_ref, 0, h_s.shape[0])
        for c in first_loads:
            c.wait()
        for at in range(0, h_s.shape[0], TILE):
            here = slice(at, at + TILE)
            mixed = sum(_dot(qkvo_s[i, 3, here, :], wo_whole[0, i * HEAD : (i + 1) * HEAD, :]) for i in range(HEADS))
            h2_s[here, :] = h_s[here, :] + mixed.astype(BF)
        dy_load.wait()

    @pl.when(s == FEEDS)
    def _():
        for c in heads(1, (0, 1, 2)):
            c.wait()
        load(10, h2_low, h2_s).start()

    @pl.when(s == EACH)
    def _():
        load(10, h2_low, h2_s).wait()
        for c in [load(0, hs[0], h_s), *heads(0, (0, 1, 2, 3))]:
            c.start()

    @pl.when(s == EACH + FEEDS)
    def _():
        for c in [load(0, hs[0], h_s), *heads(0, (0, 1, 2, 3))]:
            c.wait()

    def copy(stage, unit):
        slot = lax.rem(unit, SLOTS)
        src = (term, both, side, total, mine)[stage]
        dst = (swapped, inward, received, received, other)[stage]
        to = (partner, inner, inner, outer, partner)[stage]
        return pltpu.make_async_remote_copy(
            src_ref=src.at[lax.rem(unit, RING), 1 - core] if stage == 0 else src.at[slot], dst_ref=dst.at[slot],
            send_sem=send_sem.at[stage, slot], recv_sem=recv_sem.at[stage, slot], device_id={"dp": to}, device_id_type=pl.DeviceIdType.MESH)

    def write(unit):
        slot = lax.rem(unit, SLOTS)
        return [pltpu.make_async_copy(src.at[slot], out_ref.at[unit, to], write_sem.at[i, slot])
                for i, (src, to) in enumerate(((mine, core), (other, 1 - core)))]

    def squared(x):
        x = x.astype(F32)
        return jnp.sum((x * x).reshape(-1, 8, FB), axis=0)

    def tick(now):
        @pl.when(now > 0)
        def _():
            pl.semaphore_wait(from_partner, 1)
            pl.semaphore_wait(from_inner, 1)

            @pl.when(middle)
            def _():
                pl.semaphore_wait(from_outer, 1)

        def at(n):
            unit = now - FIRST - STARTS[n]
            safe = jnp.clip(unit, 0, UNITS - 1)
            return safe, (unit >= 0) & (unit < UNITS), lax.rem(safe, SLOTS)

        def when(n, who=None):
            unit, there, slot = at(n)
            return lambda f: pl.when(there if who is None else there & who)(functools.partial(f, unit, slot))

        @when(6)
        def _(unit, slot):
            for c in write(unit):
                c.wait()

        @when(5)
        def _(unit, slot):
            copy(4, unit).wait()
            for c in write(unit):
                c.start()
            squares[0] += squared(mine[slot])
            squares[1] += squared(other[slot])

        @when(4)
        def _(unit, slot):
            @pl.when(middle)
            def _():
                copy(3, unit).wait_send()
                mine[slot] = total[slot]

            @pl.when(end)
            def _():
                copy(3, unit).wait_recv()
                mine[slot] = received[slot]

            copy(4, unit).start()

        @when(3, middle)
        def _(unit, slot):
            copy(2, unit).wait()
            total[slot] = (side[slot].astype(F32) + received[slot].astype(F32)).astype(BF)
            copy(3, unit).start()

        @when(2, middle)
        def _(unit, slot):
            copy(1, unit).wait_recv()
            side[slot] = (wide_both[slot] + inward[slot].astype(F32)).astype(BF)
            copy(2, unit).start()

        @when(2, end)
        def _(unit, slot):
            copy(1, unit).wait_send()

        @when(1)
        def _(unit, slot):
            copy(0, unit).wait()
            terms = term[lax.rem(unit, RING), core].astype(F32) + swapped[slot].astype(F32)

            @pl.when(end)
            def _():
                both[slot] = terms.astype(BF)
                copy(1, unit).start()

            @pl.when(middle)
            def _():
                wide_both[slot] = terms

        @when(0)
        def _(unit, slot):
            copy(0, unit).start()

        @pl.when(now < LAST)
        def _():
            tell(from_partner, partner)

            @pl.when(end)
            def _():
                tell(from_outer, inner)

            @pl.when(middle)
            def _():
                tell(from_inner, inner)
                tell(from_inner, outer)

    term_now = lambda m: term.at[lax.rem(_first_unit(s) + m, RING)]
    upper = s < EACH
    n = jnp.where(upper, s - FEEDS, s - EACH - FEEDS)
    n = jnp.clip(n, 0, HEADS - 1)
    feed_parts = _feed_parts((s == 0) | (s == EACH), (s == FEEDS - 1) | (s == EACH + FEEDS - 1), wg_ref, wu_ref, wd_ref, term_now, h2_s, dh_s, b_s, bt_s,
                             dht_s, db_s, dgate_s, dup_s, act_s)
    for j in range(3):
        pl.when(_has_tick(s, j))(lambda j=j: tick(_first_tick(s) + j))
        pl.when(_is_feed(s))(feed_parts[j])

        @pl.when(_is_head(s))
        def _(j=j):
            lse = jnp.where(upper, lses[1][n], lses[0][n])
            _head_parts(n == 0, n == HEADS - 1, upper, wo_ref, wq_ref, wk_ref, wv_ref, cos_ref, sin_ref, lse, term_now,
                        *(qkvo_s.at[n, i] for i in range(4)), h_s, dh_s, bt_s, db_s, dup_s, dgate_s, dqt_s, delta_s)[j]()

    @pl.when(s == STEPS - 1)
    def _():
        both_halves = jnp.sum(squares[0], keepdims=True) + jnp.sum(squares[1], keepdims=True)
        factor = jnp.minimum(1.0, 0.5 * lax.rsqrt(both_halves * (1.0 / count) + 1e-30))
        factor_ref[...] = jnp.broadcast_to(factor, factor_ref.shape)


def _backward(dy, kept, weights, tables):
    wq, wk, wv, wo, wg, wu, wd = weights
    t, d = dy.shape
    count = sum(w.size for w in weights)

    def feed_at(s):
        return jnp.where(s < EACH, 1, 0), jnp.minimum(jnp.where(s < EACH, s, s - EACH), FEEDS - 1)

    def head_at(s):
        return jnp.where(s < EACH, 1, 0), jnp.clip(jnp.where(s < EACH, s - FEEDS, s - EACH - FEEDS), 0, HEADS - 1)

    def across(s):
        layer, n = feed_at(s)
        return layer, 0, n

    def down(s):
        layer, n = feed_at(s)
        return layer, n, 0

    def head_across(s):
        layer, n = head_at(s)
        return layer, 0, n

    def head_down(s):
        layer, n = head_at(s)
        return layer, n, 0

    hbm = pl.BlockSpec(memory_space=pltpu.HBM)
    fixed = lambda a: pl.BlockSpec(a.shape, lambda s: (0,) * a.ndim, pipeline_mode=pl.Buffered(1))
    given = [dy, kept[0][6], *(k[0] for k in kept), *kept[0][1:5], *kept[1][1:5], *(k[5] for k in kept)]
    specs = [hbm] * 12 + [fixed(k[5]) for k in kept]
    given += [wg, wu, wd, wo, wq, wk, wv, wo, *tables]
    specs += [pl.BlockSpec((1, d, FB), across)] * 2 + [pl.BlockSpec((1, FB, d), down), pl.BlockSpec((1, HEAD, d), head_down)]
    specs += [pl.BlockSpec((1, d, HEAD), head_across)] * 3
    specs += [pl.BlockSpec((1, d, d), lambda s: (1, 0, 0), pipeline_mode=pl.Buffered(1)), *(fixed(a) for a in tables)]
    tokens = pltpu.VMEM((t, d), BF)
    table = pltpu.VMEM((t, HALF), F32)
    slots = pltpu.VMEM((SLOTS, HALFB, FB), BF)
    return pl.pallas_call(
        functools.partial(_backward_kernel, count),
        grid=(STEPS,),
        in_specs=specs,
        out_specs=[hbm, pl.BlockSpec((8, 128), lambda s: (0, 0))],
        out_shape=[jax.ShapeDtypeStruct((UNITS, 2, HALFB, FB), BF), jax.ShapeDtypeStruct((8, 128), F32)],
        scratch_shapes=[table, table, tokens, tokens, tokens, pltpu.VMEM((HEADS, 4, t, HEAD), BF), tokens, pltpu.VMEM((d, t), BF), pltpu.VMEM((d, t), BF),
                        pltpu.VMEM((t, d), F32), pltpu.VMEM((t, FB), BF), pltpu.VMEM((t, FB), BF), pltpu.VMEM((t, FB), BF), pltpu.VMEM((HEAD, t), F32),
                        pltpu.VMEM((1, t), F32), pltpu.VMEM((RING, 2, HALFB, FB), BF), slots, slots, pltpu.VMEM((SLOTS, HALFB, FB), F32), slots, slots,
                        slots, slots, slots, slots,
                        pltpu.VMEM((2, 8, FB), F32),
                        pltpu.SemaphoreType.DMA((11,)), pltpu.SemaphoreType.DMA((STAGES, SLOTS)), pltpu.SemaphoreType.DMA((STAGES, SLOTS)),
                        pltpu.SemaphoreType.DMA((2, SLOTS)),
                        pltpu.SemaphoreType.REGULAR, pltpu.SemaphoreType.REGULAR, pltpu.SemaphoreType.REGULAR],
        compiler_params=pltpu.CompilerParams(dimension_semantics=("arbitrary",), vmem_limit_bytes=BIG_VMEM, collective_id=0, has_side_effects=True),
        cost_estimate=_cost(2 * (16 * t * d * 2048 + 12 * t * t * d + 16 * t * d * d), 60 * t * d),
        name="backward",
    )(*given)


def _adamw_kernel(*refs):
    w_refs, m_refs, v_refs, feeds, heads, factor_ref, outs = refs[:7], refs[7:14], refs[14:21], refs[21:24], refs[24:26], refs[26], refs[27:]
    factor = factor_ref[0:1, 0:1]

    def one(i, g):
        g = g.astype(F32) * factor
        m = 0.9 * m_refs[i][0] + 0.1 * g
        v = 0.95 * v_refs[i][0] + 0.05 * g * g
        w = w_refs[i][0].astype(F32)
        outs[i][0] = (w - 0.02 * (m * lax.rsqrt(v + 1e-8) + 0.1 * w)).astype(BF)
        outs[7 + i][0] = m
        outs[14 + i][0] = v

    for i in range(4):
        one(i, heads[i // 2][0, 0, :, (i % 2) * HEAD : (i % 2 + 1) * HEAD])
    for i in range(3):
        one(4 + i, feeds[i][0, 0])


def _adamw(factor, weights, m, v, pieces):
    layers = weights[0].shape[0]
    thin = HEAD // 2
    by_rows = pl.BlockSpec((1, thin, HEAD), lambda l, f, r: (l, (f % 2) * 2 + r, f // 2))
    by_columns = pl.BlockSpec((1, thin, HEAD), lambda l, f, r: (l, (f // 2) * 2 + r, f % 2))
    wide = pl.BlockSpec((1, HALFB, FB), lambda l, f, r: (l, r, f))
    down = pl.BlockSpec((1, HALFB, FB), lambda l, f, r: (l, 2 * f + r, 0))
    like = [by_rows, by_rows, by_rows, by_columns, wide, wide, down]
    feeds = [pl.BlockSpec((1, 1, HALFB, FB), lambda l, f, r, m=m: ((1 - l) * LAYER_UNITS + FEED_UNITS * f + m, r, 0, 0)) for m in range(FEED_UNITS)]
    heads = [pl.BlockSpec((1, 1, thin, FB), lambda l, f, r, m=m: ((1 - l) * LAYER_UNITS + FEEDS * FEED_UNITS + HEAD_UNITS * (f // 2) + m, f % 2, r, 0))
             for m in range(HEAD_UNITS)]
    return pl.pallas_call(
        _adamw_kernel,
        grid=(layers, FEEDS, 2),
        in_specs=like * 3 + feeds + heads + [pl.BlockSpec((8, 128), lambda l, f, r: (0, 0))],
        out_specs=like * 3,
        out_shape=[jax.ShapeDtypeStruct(w.shape, BF) for w in weights] + [jax.ShapeDtypeStruct(w.shape, F32) for w in weights] * 2,
        compiler_params=_params(("arbitrary",) * 3),
        cost_estimate=_cost(200 * 2**20, 180 * 2**20),
        name="adamw",
    )(*weights, *m, *v, *[pieces] * 5, factor)


def solution(mesh):
    def step(x, dy, *arrays):
        weights, m, v = (arrays[i : i + 7] for i in (0, 7, 14))
        wq, wk, wv, wo, wg, wu, wd = weights
        layers = wq.shape[0]
        h, t = x[0], x.shape[1]
        tables = _tables(t)
        kept = []
        for n in range(layers):
            q, k, val = _qkv(h, wq, wk, wv, tables, n)
            o, lse = _attend(q, k, val)
            if n < layers - 1:
                h2, h3 = _feed(h, o, wo, wg, wu, wd, n)
            else:
                h2 = h3 = None
            kept.append((h, q, k, val, o, lse, h2))
            h = h3
        pieces, factor = _backward(dy[0], kept, weights, tables)
        return tuple(_adamw(factor, weights, m, v, pieces))

    states, all_of = P(("rep", "dp"), None, None), P(None, None, None)
    return jax.shard_map(
        step,
        mesh=mesh,
        in_specs=(states, states) + (all_of,) * 21,
        out_specs=(P("rep", None, None),) * 21,
        check_vma=False,
    )
```

```python
import functools

import jax
import jax.numpy as jnp
import numpy as np
from jax import lax
from jax.experimental import pallas as pl
from jax.experimental.pallas import tpu as pltpu
from jax.sharding import PartitionSpec as P

BF, F32 = jnp.bfloat16, jnp.float32
LOG2E = 1.4426950408889634
HEAD = 256
THETA = 10000
HALF = HEAD // 2
TILE = 512
TILE_QKV = 256
FINE = 64
FB = 512
VMEM = 60 * 2**20


def _dot(a, b, ca=1, cb=0):
    return lax.dot_general(a, b, (((ca,), (cb,)), ((), ())), preferred_element_type=F32)


def _norm(h):
    wide = h.astype(F32)
    scale = lax.rsqrt(jnp.mean(wide * wide, -1, keepdims=True) + 1e-6)
    return (wide * scale).astype(BF), wide, scale


def _norm_back(by_out, wide, scale):
    by_scale = jnp.sum(by_out * wide, -1, keepdims=True)
    return by_out * scale - wide * (by_scale * scale * scale * scale * (1.0 / wide.shape[-1]))


def _turn(t, cos, sin, back=False):
    a, b = t[:, :HALF].astype(F32), t[:, HALF:].astype(F32)
    if back:
        return jnp.concatenate([a * cos + b * sin, b * cos - a * sin], -1).astype(BF)
    return jnp.concatenate([a * cos - b * sin, b * cos + a * sin], -1).astype(BF)


def _each(t, size=TILE):
    return lambda f: pl.loop(0, t // size)(lambda i: f(pl.ds(pl.multiple_of(i * size, size), size)))


def _params(semantics, **more):
    return pltpu.CompilerParams(dimension_semantics=semantics, vmem_limit_bytes=VMEM, **more)


def _cost(flops, bytes_, exps=0):
    return pl.CostEstimate(flops=int(flops), bytes_accessed=int(bytes_), transcendentals=int(exps))


def _tables(t):
    rate = THETA ** (-np.arange(HALF) / HALF)
    far, near = np.arange(0, t, FINE)[:, None] * rate, np.arange(FINE)[:, None] * rate
    return tuple(jnp.asarray(x, F32) for x in (np.cos(far), np.sin(far), np.cos(near), np.sin(near)))


def _spread(tables, cos_ref, sin_ref, first, count):
    cos_far, sin_far, cos_near, sin_near = tables
    c, s = cos_near[...], sin_near[...]
    for i in range(count // FINE):
        here = pl.ds(first // FINE + i, 1) if isinstance(first, int) else pl.ds(lax.div(first, FINE) + i, 1)
        cf, sf = cos_far[here, :], sin_far[here, :]
        cos_ref[i * FINE : (i + 1) * FINE, :] = cf * c - sf * s
        sin_ref[i * FINE : (i + 1) * FINE, :] = sf * c + cf * s


def _qkv_kernel(h_ref, wq_ref, wk_ref, wv_ref, *refs):
    tables, (q_ref, k_ref, v_ref, cos_ref, sin_ref) = refs[:4], refs[4:]
    a, _, _ = _norm(h_ref[...])
    _spread(tables, cos_ref, sin_ref, pl.program_id(0) * TILE_QKV, TILE_QKV)
    cos, sin = cos_ref[...], sin_ref[...]
    for w_ref, out in ((wq_ref, q_ref), (wk_ref, k_ref)):
        t = _dot(a, w_ref[0]).astype(BF)
        for at in range(0, t.shape[1], HEAD):
            out[:, at : at + HEAD] = _turn(t[:, at : at + HEAD], cos, sin)
    v_ref[...] = _dot(a, wv_ref[0]).astype(BF)


def _qkv(h, wq, wk, wv, tables, layer):
    t, d = h.shape
    rows = pl.BlockSpec((TILE_QKV, d), lambda i: (i, 0))
    whole = pl.BlockSpec((1, d, d), lambda i: (layer, 0, 0))
    tabled = [pl.BlockSpec(a.shape, lambda i: (0, 0)) for a in tables]
    return pl.pallas_call(
        _qkv_kernel,
        grid=(t // TILE_QKV,),
        in_specs=[rows, whole, whole, whole, *tabled],
        out_specs=[rows] * 3,
        out_shape=[jax.ShapeDtypeStruct((t, d), BF)] * 3,
        scratch_shapes=[pltpu.VMEM((TILE_QKV, HALF), F32)] * 2,
        compiler_params=_params(("arbitrary",)),
        cost_estimate=_cost(6 * t * d * d, 8 * t * d + 6 * d * d),
        name="qkv",
    )(h, wq, wk, wv, *tables)


def _attend_kernel(q_ref, k_ref, v_ref, o_ref, lse_ref, vt_s, p_s):
    t = q_ref.shape[0]
    e = HEAD**-0.5 * LOG2E
    vt_s[...] = v_ref[...].T
    hide = lax.broadcasted_iota(jnp.int32, (TILE, TILE), 0) > lax.broadcasted_iota(jnp.int32, (TILE, TILE), 1)
    for at in range(0, t, TILE):
        q = q_ref[at : at + TILE, :]
        scores = [_dot(k_ref[j : j + TILE, :], q, 1, 1) for j in range(0, at + TILE, TILE)]
        scores[-1] = jnp.where(hide, -jnp.inf, scores[-1])
        top = functools.reduce(jnp.maximum, [s.max(axis=0, keepdims=True) for s in scores])
        total = 0.0
        for n, s in enumerate(scores):
            p = jnp.exp2((s - top) * e)
            total = total + p.sum(axis=0, keepdims=True)
            p_s[n * TILE : (n + 1) * TILE, :] = p.astype(BF)
        mix = _dot(vt_s[:, : at + TILE], p_s[: at + TILE, :])
        o_ref[at : at + TILE, :] = (mix * (1.0 / total)).T.astype(BF)
        lse_ref[0, :, at : at + TILE] = top * e + jnp.log2(total)


def _attend(q, k, v):
    t, d = q.shape
    head = pl.BlockSpec((t, HEAD), lambda h: (0, h))
    return pl.pallas_call(
        _attend_kernel,
        grid=(d // HEAD,),
        in_specs=[head] * 3,
        out_specs=[head, pl.BlockSpec((1, 1, t), lambda h: (h, 0, 0))],
        out_shape=[jax.ShapeDtypeStruct((t, d), BF), jax.ShapeDtypeStruct((d // HEAD, 1, t), F32)],
        scratch_shapes=[pltpu.VMEM((HEAD, t), BF), pltpu.VMEM((t, TILE), BF)],
        compiler_params=_params(("arbitrary",)),
        cost_estimate=_cost(2.5 * t * t * d, 8 * t * d, t * t),
        name="attend",
    )(q, k, v)


def _feed_kernel(h_ref, o_ref, wo_ref, wg_ref, wu_ref, wd_ref, h2_ref, h3_ref):
    h2 = h_ref[...] + _dot(o_ref[...], wo_ref[0]).astype(BF)
    h2_ref[...] = h2
    b, _, _ = _norm(h2)
    out = 0.0
    for at in range(0, wg_ref.shape[2], FB):
        gate, up = _dot(b, wg_ref[0, :, at : at + FB]), _dot(b, wu_ref[0, :, at : at + FB])
        act = (gate * (0.5 * jnp.tanh(0.5 * gate) + 0.5) * up).astype(BF)
        out = out + _dot(act, wd_ref[0, at : at + FB, :])
    h3_ref[...] = h2 + out.astype(BF)


def _feed(h, o, wo, wg, wu, wd, layer):
    t, d = h.shape
    f = wg.shape[2]
    rows = pl.BlockSpec((TILE, d), lambda i: (i, 0))
    whole = lambda *shape: pl.BlockSpec((1, *shape), lambda i: (layer, 0, 0))
    return pl.pallas_call(
        _feed_kernel,
        grid=(t // TILE,),
        in_specs=[rows, rows, whole(d, d), whole(d, f), whole(d, f), whole(f, d)],
        out_specs=[rows, rows],
        out_shape=[jax.ShapeDtypeStruct((t, d), BF)] * 2,
        compiler_params=_params(("arbitrary",)),
        cost_estimate=_cost(2 * t * d * d + 6 * t * d * f, 8 * t * d + 6 * d * f, t * f),
        name="feed",
    )(h, o, wo, wg, wu, wd)


FEEDS, HEADS = 4, 2
EACH = FEEDS + HEADS
PIECES = 2 * EACH
FEED_UNITS, HEAD_UNITS = 3, 2
LAYER_UNITS = FEEDS * FEED_UNITS + HEADS * HEAD_UNITS
UNITS = 2 * LAYER_UNITS
FIRST = 3
STARTS = (0, 1, 3, 5, 7, 9, 10)
STAGES = 5
SLOTS = 4
RING = 6
LAST = UNITS - 1 + FIRST + STARTS[-1]
STEPS = PIECES + (LAST + 1 - UNITS + 2) // 3
HALFB = FB // 2
BIG_VMEM = 67043328


def _first_tick(s):
    layer = lax.div(s, EACH)
    return jnp.where(s < PIECES, layer * LAYER_UNITS + lax.div(5 * (s - layer * EACH) + 1, 2), UNITS + 3 * (s - PIECES))


def _has_tick(s, j):
    if j == 0:
        return s >= 0
    usual = _first_tick(s) + j <= LAST
    if j == 1:
        return usual
    r = lax.rem(s, EACH)
    return usual & ((s >= PIECES) | ((r != 1) & (r != 3)))


def _first_unit(s):
    layer = lax.div(s, EACH)
    r = s - layer * EACH
    return layer * LAYER_UNITS + jnp.where(r < FEEDS, FEED_UNITS * r, FEEDS * FEED_UNITS + HEAD_UNITS * (r - FEEDS))


def _is_feed(p):
    return ((p >= 0) & (p < FEEDS)) | ((p >= EACH) & (p < EACH + FEEDS))


def _is_head(p):
    return ((p >= FEEDS) & (p < EACH)) | ((p >= EACH + FEEDS) & (p < PIECES))


def _feed_parts(first, last, wg_ref, wu_ref, wd_ref, term, h2_s, dh_s, b_s, bt_s, dht_s, db_s, dgate_s, dup_s, act_s):
    t = h2_s.shape[0]
    tiles = [slice(at, at + TILE) for at in range(0, t, TILE)]

    def run(some):
        wg, wu, wd = wg_ref[0], wu_ref[0], wd_ref[0]
        for here in some:
            b = b_s[here, :]
            gate, up = _dot(b, wg), _dot(b, wu)
            dact = _dot(dh_s[here, :], wd, 1, 1).astype(BF).astype(F32)
            sig = 0.5 * jnp.tanh(0.5 * gate) + 0.5
            silu = gate * sig
            act_s[here, :] = (silu * up).astype(BF)
            dup = (dact * silu).astype(BF)
            dgate = (dact * up * (sig + silu * (1.0 - sig))).astype(BF)
            dup_s[here, :] = dup
            dgate_s[here, :] = dgate
            db_s[here, :] += _dot(dgate, wg, 1, 1) + _dot(dup, wu, 1, 1)

    def one():
        @pl.when(first)
        def _():
            @_each(t)
            def _(here):
                b, _, _ = _norm(h2_s[here, :])
                b_s[here, :] = b
                bt_s[:, here] = b.T
                dht_s[:, here] = dh_s[here, :].T
                db_s[here, :] = jnp.zeros((TILE, db_s.shape[1]), F32)

        run(tiles[: len(tiles) // 2])

    def two():
        run(tiles[len(tiles) // 2 :])

    def three():
        for m, dw in enumerate((_dot(bt_s[...], dgate_s[...]), _dot(bt_s[...], dup_s[...]), _dot(dht_s[...], act_s[...]).T)):
            dw = dw.astype(BF)
            term(m)[0] = dw[:HALFB, :]
            term(m)[1] = dw[HALFB:, :]

        @pl.when(last)
        def _():
            @_each(t)
            def _(here):
                _, wide, scale = _norm(h2_s[here, :])
                dh_s[here, :] = dh_s[here, :] + _norm_back(db_s[here, :], wide, scale).astype(BF)

    return one, two, three


def _head_parts(first, last, with_dh, wo_ref, wq_ref, wk_ref, wv_ref, cos_ref, sin_ref, lse, term, q_ref, k_ref, v_ref, o_ref, h_s, dh_s, at_s, da_s,
                do_s, dkv_s, dqt_s, delta_s):
    t = h_s.shape[0]
    scale = HEAD**-0.5
    e = scale * LOG2E
    tiles = [slice(at, at + TILE) for at in range(0, t, TILE)]

    def put(m, half, x):
        term(m // 2)[half, :, (m % 2) * HEAD : (m % 2 + 1) * HEAD] = x

    def run(some):
        hide = lax.broadcasted_iota(jnp.int32, (TILE, TILE), 0) > lax.broadcasted_iota(jnp.int32, (TILE, TILE), 1)
        for tile in some:
            at = tile.start
            k, v = k_ref[tile, :], v_ref[tile, :]
            kt = k.T
            ps, dss = [], []
            for i in range(at, t, TILE):
                here = slice(i, i + TILE)
                p = jnp.exp2(_dot(k, q_ref[here, :], 1, 1) * e - lse[:, here])
                if i == at:
                    p = jnp.where(hide, 0.0, p)
                ds = (p * (_dot(v, do_s[here, :HEAD], 1, 1) - delta_s[:, here])).astype(BF)
                ps.append(p.astype(BF))
                dss.append(ds)
            p, ds = jnp.concatenate(ps, axis=1), jnp.concatenate(dss, axis=1)
            dkv_s[tile, :HEAD] = (_dot(ds, q_ref[at:, :]) * scale).astype(BF)
            dkv_s[tile, HEAD:] = _dot(p, do_s[at:, :HEAD]).astype(BF)
            dq = _dot(kt, ds)
            dqt_s[:, at:] = dq if at == 0 else dqt_s[:, at:] + dq

    def one():
        @pl.when(first)
        def _():
            @_each(t)
            def _(here):
                at_s[:, here] = _norm(h_s[here, :])[0].T
                da_s[here, :] = jnp.zeros((TILE, da_s.shape[1]), F32)

        @_each(t)
        def _(here):
            do = _dot(dh_s[here, :], wo_ref[0], 1, 1).astype(BF)
            do_s[here, :HEAD] = do
            both = do.astype(F32) * o_ref[here, :].astype(F32)
            delta_s[:, here] = (both[:, :HALF] + both[:, HALF:]).T.sum(axis=0, keepdims=True)
        run(tiles[:1])

    def two():
        run(tiles[1:])

    def three():
        dwo = _dot(o_ref[...].T, dh_s[...]).astype(BF)
        put(3, 0, dwo[:, :HEAD])
        put(3, 1, dwo[:, HEAD:])
        for m, w_ref in enumerate((wq_ref, wk_ref, wv_ref)):
            parts = []
            for here in tiles:
                part = (dqt_s[:, here] * scale).T.astype(BF) if m == 0 else dkv_s[here, (m - 1) * HEAD : m * HEAD]
                parts.append(_turn(part, cos_ref[here, :], sin_ref[here, :], True) if m < 2 else part)
            part = jnp.concatenate(parts, axis=0)
            dw = _dot(at_s[...], part).astype(BF)
            put(m, 0, dw[:HEAD, :])
            put(m, 1, dw[HEAD:, :])

            @pl.when(with_dh)
            def _():
                da_s[...] += _dot(part, w_ref[0], 1, 1)

        @pl.when(with_dh & last)
        def _():
            @_each(t)
            def _(here):
                _, wide, s = _norm(h_s[here, :])
                dh_s[here, :] = dh_s[here, :] + _norm_back(da_s[here, :], wide, s).astype(BF)

    return one, two, three


def _backward_kernel(count, *refs):
    (dy, h2_low, hs, qkvo, lses) = refs[0], refs[1], refs[2:4], (refs[4:8], refs[8:12]), refs[12:14]
    wg_ref, wu_ref, wd_ref, wo_ref, wq_ref, wk_ref, wv_ref, wo_whole = refs[14:22]
    tables, out_ref, factor_ref = refs[22:26], refs[26], refs[27]
    (cos_ref, sin_ref, h2_s, dh_s, h_s, qkvo_s, b_s, bt_s, dht_s, db_s, dgate_s, dup_s, act_s, dqt_s, delta_s,
     term, swapped, both, wide_both, inward, side, received, total, mine, other, squares,
     load_sem, send_sem, recv_sem, write_sem, from_partner, from_inner, from_outer) = refs[28:]
    s = pl.program_id(0)
    me = lax.axis_index("dp")
    core, chip = lax.rem(me, 2), lax.div(me, 2)
    partner = me + 1 - 2 * core
    end = (chip == 0) | (chip == 3)
    middle = (chip == 1) | (chip == 2)
    inner = jnp.where(chip < 2, me + 2, me - 2)
    outer = jnp.where(chip == 1, me - 2, jnp.where(chip == 2, me + 2, inner))

    def tell(semaphore, device):
        pl.semaphore_signal(semaphore, inc=1, device_id={"dp": device}, device_id_type=pl.DeviceIdType.MESH)

    def load(n, src, dst):
        return pltpu.make_async_copy(src, dst, load_sem.at[n])

    def heads(layer, which):
        return [load(1 + 4 * n + i, qkvo[layer][i].at[:, n * HEAD : (n + 1) * HEAD], qkvo_s.at[n, i]) for n in range(HEADS) for i in which]

    @pl.when(s == 0)
    def _():
        dy_load = load(9, dy, dh_s)
        first_loads = [load(0, hs[1], h_s), *heads(1, (3,))]
        for c in [*first_loads, dy_load, *heads(1, (0, 1, 2))]:
            c.start()
        barrier = pltpu.get_barrier_semaphore()
        tell(barrier, partner)
        tell(barrier, inner)

        @pl.when(middle)
        def _():
            tell(barrier, outer)
            pl.semaphore_wait(barrier, 3)

        @pl.when(end)
        def _():
            pl.semaphore_wait(barrier, 2)

        squares[...] = jnp.zeros_like(squares)
        _spread(tables, cos_ref, sin_ref, 0, h_s.shape[0])
        for c in first_loads:
            c.wait()
        @_each(h_s.shape[0])
        def _(here):
            mixed = sum(_dot(qkvo_s[i, 3, here, :], wo_whole[0, i * HEAD : (i + 1) * HEAD, :]) for i in range(HEADS))
            h2_s[here, :] = h_s[here, :] + mixed.astype(BF)
        dy_load.wait()

    @pl.when(s == FEEDS)
    def _():
        for c in heads(1, (0, 1, 2)):
            c.wait()
        load(10, h2_low, h2_s).start()

    @pl.when(s == EACH)
    def _():
        load(10, h2_low, h2_s).wait()
        for c in [load(0, hs[0], h_s), *heads(0, (0, 1, 2, 3))]:
            c.start()

    @pl.when(s == EACH + FEEDS)
    def _():
        for c in [load(0, hs[0], h_s), *heads(0, (0, 1, 2, 3))]:
            c.wait()

    def copy(stage, unit):
        slot = lax.rem(unit, SLOTS)
        src = (term, both, side, total, mine)[stage]
        dst = (swapped, inward, received, received, other)[stage]
        to = (partner, inner, inner, outer, partner)[stage]
        return pltpu.make_async_remote_copy(
            src_ref=src.at[lax.rem(unit, RING), 1 - core] if stage == 0 else src.at[slot], dst_ref=dst.at[slot],
            send_sem=send_sem.at[stage, slot], recv_sem=recv_sem.at[stage, slot], device_id={"dp": to}, device_id_type=pl.DeviceIdType.MESH)

    def write(unit):
        slot = lax.rem(unit, SLOTS)
        return [pltpu.make_async_copy(src.at[slot], out_ref.at[unit, to], write_sem.at[i, slot])
                for i, (src, to) in enumerate(((mine, core), (other, 1 - core)))]

    def squared(x):
        x = x.astype(F32)
        return jnp.sum((x * x).reshape(-1, 8, FB), axis=0)

    def tick(now):
        @pl.when(now > 0)
        def _():
            pl.semaphore_wait(from_partner, 1)
            pl.semaphore_wait(from_inner, 1)

            @pl.when(middle)
            def _():
                pl.semaphore_wait(from_outer, 1)

        def at(n):
            unit = now - FIRST - STARTS[n]
            safe = jnp.clip(unit, 0, UNITS - 1)
            return safe, (unit >= 0) & (unit < UNITS), lax.rem(safe, SLOTS)

        def when(n, who=None):
            unit, there, slot = at(n)
            return lambda f: pl.when(there if who is None else there & who)(functools.partial(f, unit, slot))

        @when(6)
        def _(unit, slot):
            for c in write(unit):
                c.wait()

        @when(5)
        def _(unit, slot):
            copy(4, unit).wait()
            for c in write(unit):
                c.start()
            squares[0] += squared(mine[slot])
            squares[1] += squared(other[slot])

        @when(4)
        def _(unit, slot):
            @pl.when(middle)
            def _():
                copy(3, unit).wait_send()
                mine[slot] = total[slot]

            @pl.when(end)
            def _():
                copy(3, unit).wait_recv()
                mine[slot] = received[slot]

            copy(4, unit).start()

        @when(3, middle)
        def _(unit, slot):
            copy(2, unit).wait()
            total[slot] = (side[slot].astype(F32) + received[slot].astype(F32)).astype(BF)
            copy(3, unit).start()

        @when(2, middle)
        def _(unit, slot):
            copy(1, unit).wait_recv()
            side[slot] = (wide_both[slot] + inward[slot].astype(F32)).astype(BF)
            copy(2, unit).start()

        @when(2, end)
        def _(unit, slot):
            copy(1, unit).wait_send()

        @when(1)
        def _(unit, slot):
            copy(0, unit).wait()
            terms = term[lax.rem(unit, RING), core].astype(F32) + swapped[slot].astype(F32)

            @pl.when(end)
            def _():
                both[slot] = terms.astype(BF)
                copy(1, unit).start()

            @pl.when(middle)
            def _():
                wide_both[slot] = terms

        @when(0)
        def _(unit, slot):
            copy(0, unit).start()

        @pl.when(now < LAST)
        def _():
            tell(from_partner, partner)

            @pl.when(end)
            def _():
                tell(from_outer, inner)

            @pl.when(middle)
            def _():
                tell(from_inner, inner)
                tell(from_inner, outer)

    term_now = lambda m: term.at[lax.rem(_first_unit(s) + m, RING)]
    upper = s < EACH
    n = jnp.where(upper, s - FEEDS, s - EACH - FEEDS)
    n = jnp.clip(n, 0, HEADS - 1)
    feed_parts = _feed_parts((s == 0) | (s == EACH), (s == FEEDS - 1) | (s == EACH + FEEDS - 1), wg_ref, wu_ref, wd_ref, term_now, h2_s, dh_s, b_s, bt_s,
                             dht_s, db_s, dgate_s, dup_s, act_s)
    for j in range(3):
        pl.when(_has_tick(s, j))(lambda j=j: tick(_first_tick(s) + j))
        pl.when(_is_feed(s))(feed_parts[j])

        @pl.when(_is_head(s))
        def _(j=j):
            lse = jnp.where(upper, lses[1][n], lses[0][n])
            _head_parts(n == 0, n == HEADS - 1, upper, wo_ref, wq_ref, wk_ref, wv_ref, cos_ref, sin_ref, lse, term_now,
                        *(qkvo_s.at[n, i] for i in range(4)), h_s, dh_s, bt_s, db_s, dup_s, dgate_s, dqt_s, delta_s)[j]()

    @pl.when(s == STEPS - 1)
    def _():
        both_halves = jnp.sum(squares[0], keepdims=True) + jnp.sum(squares[1], keepdims=True)
        factor = jnp.minimum(1.0, 0.5 * lax.rsqrt(both_halves * (1.0 / count) + 1e-30))
        factor_ref[...] = jnp.broadcast_to(factor, factor_ref.shape)


def _backward(dy, kept, weights, tables):
    wq, wk, wv, wo, wg, wu, wd = weights
    t, d = dy.shape
    count = sum(w.size for w in weights)

    def feed_at(s):
        return jnp.where(s < EACH, 1, 0), jnp.minimum(jnp.where(s < EACH, s, s - EACH), FEEDS - 1)

    def head_at(s):
        return jnp.where(s < EACH, 1, 0), jnp.clip(jnp.where(s < EACH, s - FEEDS, s - EACH - FEEDS), 0, HEADS - 1)

    def across(s):
        layer, n = feed_at(s)
        return layer, 0, n

    def down(s):
        layer, n = feed_at(s)
        return layer, n, 0

    def head_across(s):
        layer, n = head_at(s)
        return layer, 0, n

    def head_down(s):
        layer, n = head_at(s)
        return layer, n, 0

    hbm = pl.BlockSpec(memory_space=pltpu.HBM)
    fixed = lambda a: pl.BlockSpec(a.shape, lambda s: (0,) * a.ndim, pipeline_mode=pl.Buffered(1))
    given = [dy, kept[0][6], *(k[0] for k in kept), *kept[0][1:5], *kept[1][1:5], *(k[5] for k in kept)]
    specs = [hbm] * 12 + [fixed(k[5]) for k in kept]
    given += [wg, wu, wd, wo, wq, wk, wv, wo, *tables]
    specs += [pl.BlockSpec((1, d, FB), across)] * 2 + [pl.BlockSpec((1, FB, d), down), pl.BlockSpec((1, HEAD, d), head_down)]
    specs += [pl.BlockSpec((1, d, HEAD), head_across)] * 3
    specs += [pl.BlockSpec((1, d, d), lambda s: (1, 0, 0), pipeline_mode=pl.Buffered(1)), *(fixed(a) for a in tables)]
    tokens = pltpu.VMEM((t, d), BF)
    table = pltpu.VMEM((t, HALF), F32)
    slots = pltpu.VMEM((SLOTS, HALFB, FB), BF)
    return pl.pallas_call(
        functools.partial(_backward_kernel, count),
        grid=(STEPS,),
        in_specs=specs,
        out_specs=[hbm, pl.BlockSpec((8, 128), lambda s: (0, 0))],
        out_shape=[jax.ShapeDtypeStruct((UNITS, 2, HALFB, FB), BF), jax.ShapeDtypeStruct((8, 128), F32)],
        scratch_shapes=[table, table, tokens, tokens, tokens, pltpu.VMEM((HEADS, 4, t, HEAD), BF), tokens, pltpu.VMEM((d, t), BF), pltpu.VMEM((d, t), BF),
                        pltpu.VMEM((t, d), F32), pltpu.VMEM((t, FB), BF), pltpu.VMEM((t, FB), BF), pltpu.VMEM((t, FB), BF), pltpu.VMEM((HEAD, t), F32),
                        pltpu.VMEM((1, t), F32), pltpu.VMEM((RING, 2, HALFB, FB), BF), slots, slots, pltpu.VMEM((SLOTS, HALFB, FB), F32), slots, slots,
                        slots, slots, slots, slots,
                        pltpu.VMEM((2, 8, FB), F32),
                        pltpu.SemaphoreType.DMA((11,)), pltpu.SemaphoreType.DMA((STAGES, SLOTS)), pltpu.SemaphoreType.DMA((STAGES, SLOTS)),
                        pltpu.SemaphoreType.DMA((2, SLOTS)),
                        pltpu.SemaphoreType.REGULAR, pltpu.SemaphoreType.REGULAR, pltpu.SemaphoreType.REGULAR],
        compiler_params=pltpu.CompilerParams(dimension_semantics=("arbitrary",), vmem_limit_bytes=BIG_VMEM, collective_id=0, has_side_effects=True),
        cost_estimate=_cost(2 * (16 * t * d * 2048 + 12 * t * t * d + 16 * t * d * d), 60 * t * d),
        name="backward",
    )(*given)


def _adamw_kernel(*refs):
    w_refs, m_refs, v_refs, feeds, heads, factor_ref, outs = refs[:7], refs[7:14], refs[14:21], refs[21:24], refs[24:26], refs[26], refs[27:]
    factor = factor_ref[0:1, 0:1]

    def one(i, here, g):
        g = g.astype(F32) * factor
        m = 0.9 * m_refs[i][0, here] + 0.1 * g
        v = 0.95 * v_refs[i][0, here] + 0.05 * g * g
        w = w_refs[i][0, here].astype(F32)
        outs[i][0, here] = (w - 0.02 * (m * lax.rsqrt(v + 1e-8) + 0.1 * w)).astype(BF)
        outs[7 + i][0, here] = m
        outs[14 + i][0, here] = v

    @_each(HEAD // 2, 32)
    def _(here):
        for i in range(4):
            one(i, here, heads[i // 2][0, 0, here, (i % 2) * HEAD : (i % 2 + 1) * HEAD])

    @_each(HALFB, 32)
    def _(here):
        for i in range(3):
            one(4 + i, here, feeds[i][0, 0, here])


def _adamw(factor, weights, m, v, pieces):
    layers = weights[0].shape[0]
    thin = HEAD // 2
    by_rows = pl.BlockSpec((1, thin, HEAD), lambda l, f, r: (l, (f % 2) * 2 + r, f // 2))
    by_columns = pl.BlockSpec((1, thin, HEAD), lambda l, f, r: (l, (f // 2) * 2 + r, f % 2))
    wide = pl.BlockSpec((1, HALFB, FB), lambda l, f, r: (l, r, f))
    down = pl.BlockSpec((1, HALFB, FB), lambda l, f, r: (l, 2 * f + r, 0))
    like = [by_rows, by_rows, by_rows, by_columns, wide, wide, down]
    feeds = [pl.BlockSpec((1, 1, HALFB, FB), lambda l, f, r, m=m: ((1 - l) * LAYER_UNITS + FEED_UNITS * f + m, r, 0, 0)) for m in range(FEED_UNITS)]
    heads = [pl.BlockSpec((1, 1, thin, FB), lambda l, f, r, m=m: ((1 - l) * LAYER_UNITS + FEEDS * FEED_UNITS + HEAD_UNITS * (f // 2) + m, f % 2, r, 0))
             for m in range(HEAD_UNITS)]
    return pl.pallas_call(
        _adamw_kernel,
        grid=(layers, FEEDS, 2),
        in_specs=like * 3 + feeds + heads + [pl.BlockSpec((8, 128), lambda l, f, r: (0, 0))],
        out_specs=like * 3,
        out_shape=[jax.ShapeDtypeStruct(w.shape, BF) for w in weights] + [jax.ShapeDtypeStruct(w.shape, F32) for w in weights] * 2,
        compiler_params=_params(("arbitrary",) * 3),
        cost_estimate=_cost(200 * 2**20, 180 * 2**20),
        name="adamw",
    )(*weights, *m, *v, *[pieces] * 5, factor)


def solution(mesh):
    def step(x, dy, *arrays):
        weights, m, v = (arrays[i : i + 7] for i in (0, 7, 14))
        wq, wk, wv, wo, wg, wu, wd = weights
        layers = wq.shape[0]
        h, t = x[0], x.shape[1]
        tables = _tables(t)
        kept = []
        for n in range(layers):
            q, k, val = _qkv(h, wq, wk, wv, tables, n)
            o, lse = _attend(q, k, val)
            if n < layers - 1:
                h2, h3 = _feed(h, o, wo, wg, wu, wd, n)
            else:
                h2 = h3 = None
            kept.append((h, q, k, val, o, lse, h2))
            h = h3
        pieces, factor = _backward(dy[0], kept, weights, tables)
        return tuple(_adamw(factor, weights, m, v, pieces))

    states, all_of = P(("rep", "dp"), None, None), P(None, None, None)
    return jax.shard_map(
        step,
        mesh=mesh,
        in_specs=(states, states) + (all_of,) * 21,
        out_specs=(P("rep", None, None),) * 21,
        check_vma=False,
    )
```
